32 devices in a mesh: dp: 4 (over y, z), tp: 8 (over x, core).
Axes of the slice: x: 4, y: 2, z: 2, core: 2. Of those that a mesh axis runs over, the one named last changes fastest.
The devices are a block of a 4x4x8 slice.
Arguments:
- x: bfloat16 [8, 512, 4096], P('dp', 'tp'), parts along dimension 0
- start: int32 [8], P('dp'), parts along dimension 0
- k_local: bfloat16 [8, 4096, 8, 128], P('dp', None, 'tp'), parts along dimension 0
- v_local: bfloat16 [8, 4096, 8, 128], P('dp', None, 'tp'), parts along dimension 0
- k_global: bfloat16 [8, 4608, 8, 128], P('dp', None, 'tp'), parts along dimension 0
- v_global: bfloat16 [8, 4608, 8, 128], P('dp', None, 'tp'), parts along dimension 0
- norms: float32 [2, 4, 4096], replicated
- w_q: bfloat16 [2, 4096, 4096], P(None, None, 'tp')
- w_k: bfloat16 [2, 4096, 1024], P(None, None, 'tp')
- w_v: bfloat16 [2, 4096, 1024], P(None, None, 'tp')
- w_o: bfloat16 [2, 4096, 4096], P(None, 'tp')
- w_gate: bfloat16 [2, 4096, 14336], P(None, None, 'tp')
- w_up: bfloat16 [2, 4096, 14336], P(None, None, 'tp')
- w_down: bfloat16 [2, 14336, 4096], P(None, 'tp')
Outputs:
- output 1: bfloat16 [8, 512, 4096], P('dp', 'tp'), parts along dimension 0
- output 2: bfloat16 [8, 4096, 8, 128], P('dp', None, 'tp'), parts along dimension 0
- output 3: bfloat16 [8, 4096, 8, 128], P('dp', None, 'tp'), parts along dimension 0
- output 4: bfloat16 [8, 4608, 8, 128], P('dp', None, 'tp'), parts along dimension 0
- output 5: bfloat16 [8, 4608, 8, 128], P('dp', None, 'tp'), parts along dimension 0
There are 4 independent parts. The reference program is written for one: setup_inputs(seed, part) draws one part's arguments, and reference() takes and returns one part's arrays. A program takes and returns all parts, laid end to end along the dimension named above; an argument that names none is the same for every part.
All inputs are finite; a program needn't handle non-finite values.
Results may differ from the reference program's by a relative error of at most 0.02.
Values are sent between devices in bfloat16 or wider.
A program may use at most 768 MiB of HBM per device.

```python
import jax
import jax.numpy as jnp
from jax import lax

BATCH_SEQS = 2
CHUNK_LEN = 512
PAST_MAX = 4096
D_MODEL = 4096
NUM_HEADS = 32
NUM_KV_HEADS = 8
HEAD_DIM = 128
FFN_DIM = 14336
WINDOW_LEN = 4096

CACHE_LEN = PAST_MAX + CHUNK_LEN
QUERY_BLOCK = min(CHUNK_LEN, 64)
QUERY_SCALE = HEAD_DIM ** -0.5
SOFT_CAP = 50.0
NORM_EPS = 1e-6
ROPE_BASE = 10000.0


def setup_inputs(seed: int = 0, part: int = 0) -> dict:
    part_keys = jax.random.split(jax.random.fold_in(jax.random.key(seed), part), 8)
    shared_keys = jax.random.split(jax.random.key(seed + 1), 9)
    q_width = NUM_HEADS * HEAD_DIM
    kv_width = NUM_KV_HEADS * HEAD_DIM
    local_shape = (BATCH_SEQS, WINDOW_LEN, NUM_KV_HEADS, HEAD_DIM)
    global_shape = (BATCH_SEQS, CACHE_LEN, NUM_KV_HEADS, HEAD_DIM)
    start_draw = jax.random.randint(part_keys[1], (BATCH_SEQS,), PAST_MAX // 2, PAST_MAX + 1, dtype=jnp.int32)
    top_seq = jax.random.randint(part_keys[2], (), 0, BATCH_SEQS, dtype=jnp.int32)
    start = jnp.where(jnp.arange(BATCH_SEQS, dtype=jnp.int32) == top_seq, PAST_MAX, start_draw).astype(jnp.int32)
    return {
        'x': jax.random.normal(part_keys[0], (BATCH_SEQS, CHUNK_LEN, D_MODEL), jnp.float32).astype(jnp.bfloat16),
        'start': start,
        'k_local': jax.random.normal(part_keys[3], local_shape, jnp.float32).astype(jnp.bfloat16),
        'v_local': jax.random.normal(part_keys[4], local_shape, jnp.float32).astype(jnp.bfloat16),
        'k_global': jax.random.normal(part_keys[5], global_shape, jnp.float32).astype(jnp.bfloat16),
        'v_global': jax.random.normal(part_keys[6], global_shape, jnp.float32).astype(jnp.bfloat16),
        'norms': 0.25 * jax.random.normal(shared_keys[0], (2, 4, D_MODEL), jnp.float32),
        'w_q': (jax.random.normal(shared_keys[1], (2, D_MODEL, q_width), jnp.float32) * D_MODEL ** -0.5).astype(jnp.bfloat16),
        'w_k': (jax.random.normal(shared_keys[2], (2, D_MODEL, kv_width), jnp.float32) * D_MODEL ** -0.5).astype(jnp.bfloat16),
        'w_v': (jax.random.normal(shared_keys[3], (2, D_MODEL, kv_width), jnp.float32) * D_MODEL ** -0.5).astype(jnp.bfloat16),
        'w_o': (jax.random.normal(shared_keys[4], (2, q_width, D_MODEL), jnp.float32) * q_width ** -0.5).astype(jnp.bfloat16),
        'w_gate': (jax.random.normal(shared_keys[5], (2, D_MODEL, FFN_DIM), jnp.float32) * D_MODEL ** -0.5).astype(jnp.bfloat16),
        'w_up': (jax.random.normal(shared_keys[6], (2, D_MODEL, FFN_DIM), jnp.float32) * D_MODEL ** -0.5).astype(jnp.bfloat16),
        'w_down': (jax.random.normal(shared_keys[7], (2, FFN_DIM, D_MODEL), jnp.float32) * FFN_DIM ** -0.5).astype(jnp.bfloat16),
    }


def rms_norm(hidden, scale):
    hidden_f32 = hidden.astype(jnp.float32)
    inv_rms = lax.rsqrt(jnp.mean(hidden_f32 * hidden_f32, axis=-1, keepdims=True) + NORM_EPS)
    return hidden_f32 * inv_rms * (1.0 + scale)


def rope_apply(projected, positions):
    half_dim = projected.shape[-1] // 2
    inv_freq = ROPE_BASE ** (jnp.arange(half_dim, dtype=jnp.float32) * (-2.0 / projected.shape[-1]))
    angles = positions.astype(jnp.float32)[..., None] * inv_freq
    cos_tab = jnp.cos(angles)[..., None, :]
    sin_tab = jnp.sin(angles)[..., None, :]
    lead_half = projected[..., :half_dim]
    tail_half = projected[..., half_dim:]
    return jnp.concatenate([lead_half * cos_tab - tail_half * sin_tab, tail_half * cos_tab + lead_half * sin_tab], axis=-1)


def window_positions(start, window):
    slot_ids = jnp.arange(window, dtype=jnp.int32)
    last_pos = start[:, None] - 1
    return last_pos - jnp.remainder(last_pos - slot_ids[None, :], window)


def window_write(cache, fresh, start):
    window = cache.shape[1]
    chunk_len = fresh.shape[1]
    keep_len = min(chunk_len, window)
    tail_rows = jnp.pad(fresh[:, chunk_len - keep_len:], ((0, 0), (0, window - keep_len), (0, 0), (0, 0)))
    first_pos = start + (chunk_len - keep_len)
    rolled = jax.vmap(lambda rows, amount: jnp.roll(rows, amount, axis=0))(tail_rows, jnp.remainder(first_pos, window))
    slot_ids = jnp.arange(window, dtype=jnp.int32)
    written = jnp.remainder(slot_ids[None, :] - first_pos[:, None], window) < keep_len
    return jnp.where(written[:, :, None, None], rolled, cache)


def linear_write(cache, fresh, start):
    return jax.vmap(lambda rows, new_rows, offset: lax.dynamic_update_slice_in_dim(rows, new_rows, offset, axis=0))(cache, fresh, start)


def attend_seq(q_seq, k_seq, v_seq, q_pos, k_pos, window):
    chunk_len, heads, head_dim = q_seq.shape
    kv_heads = k_seq.shape[1]
    keys_f32 = k_seq.astype(jnp.float32)
    vals_f32 = v_seq.astype(jnp.float32)
    q_blocks = q_seq.reshape(chunk_len // QUERY_BLOCK, QUERY_BLOCK, kv_heads, heads // kv_heads, head_dim)
    pos_blocks = q_pos.reshape(chunk_len // QUERY_BLOCK, QUERY_BLOCK)

    def one_block(item):
        q_blk, p_blk = item
        scores = jnp.einsum('qkgd,tkd->kgqt', q_blk.astype(jnp.float32), keys_f32) * QUERY_SCALE
        capped = SOFT_CAP * jnp.tanh(scores / SOFT_CAP)
        allowed = k_pos[None, :] <= p_blk[:, None]
        if window > 0:
            allowed = allowed & (k_pos[None, :] > p_blk[:, None] - window) & (k_pos[None, :] >= 0)
        masked = jnp.where(allowed, capped, -1e30)
        weights = jnp.exp(masked - jnp.max(masked, axis=-1, keepdims=True))
        probs = (weights / jnp.sum(weights, axis=-1, keepdims=True)).astype(jnp.bfloat16)
        block_out = jnp.einsum('kgqt,tkd->qkgd', probs.astype(jnp.float32), vals_f32)
        return block_out.astype(jnp.bfloat16)

    all_blocks = lax.map(one_block, (q_blocks, pos_blocks))
    return all_blocks.reshape(chunk_len, heads * head_dim)


def attention_half(hidden, start, k_cache, v_cache, norm_pre, norm_post, w_q, w_k, w_v, w_o, is_local):
    num_seqs = hidden.shape[0]
    positions = start[:, None] + jnp.arange(CHUNK_LEN, dtype=jnp.int32)[None, :]
    flat = rms_norm(hidden, norm_pre).astype(jnp.bfloat16).reshape(num_seqs * CHUNK_LEN, D_MODEL)
    q_proj = jnp.dot(flat, w_q, preferred_element_type=jnp.float32).reshape(num_seqs, CHUNK_LEN, NUM_HEADS, HEAD_DIM)
    k_proj = jnp.dot(flat, w_k, preferred_element_type=jnp.float32).reshape(num_seqs, CHUNK_LEN, NUM_KV_HEADS, HEAD_DIM)
    v_proj = jnp.dot(flat, w_v, preferred_element_type=jnp.float32).reshape(num_seqs, CHUNK_LEN, NUM_KV_HEADS, HEAD_DIM)
    q_rot = rope_apply(q_proj, positions).astype(jnp.bfloat16)
    k_new = rope_apply(k_proj, positions).astype(jnp.bfloat16)
    v_new = v_proj.astype(jnp.bfloat16)
    k_old = k_cache.astype(k_new.dtype)
    v_old = v_cache.astype(v_new.dtype)
    if is_local:
        window = WINDOW_LEN
        k_keys = jnp.concatenate([k_old, k_new], axis=1)
        v_keys = jnp.concatenate([v_old, v_new], axis=1)
        key_pos = jnp.concatenate([window_positions(start, WINDOW_LEN), positions], axis=1)
        k_next = window_write(k_old, k_new, start)
        v_next = window_write(v_old, v_new, start)
    else:
        window = 0
        k_next = linear_write(k_old, k_new, start)
        v_next = linear_write(v_old, v_new, start)
        k_keys = k_next
        v_keys = v_next
        key_pos = jnp.broadcast_to(jnp.arange(CACHE_LEN, dtype=jnp.int32)[None, :], (num_seqs, CACHE_LEN))
    mixed = lax.map(lambda item: attend_seq(item[0], item[1], item[2], item[3], item[4], window), (q_rot, k_keys, v_keys, positions, key_pos))
    attn_out = jnp.dot(mixed.reshape(num_seqs * CHUNK_LEN, NUM_HEADS * HEAD_DIM), w_o, preferred_element_type=jnp.float32).astype(jnp.bfloat16)
    attn_out = attn_out.reshape(num_seqs, CHUNK_LEN, D_MODEL)
    x_next = (hidden.astype(jnp.float32) + rms_norm(attn_out, norm_post)).astype(jnp.bfloat16)
    return x_next, k_next, v_next


def mlp_half(hidden, norm_pre, norm_post, w_gate, w_up, w_down):
    num_seqs = hidden.shape[0]
    flat = rms_norm(hidden, norm_pre).astype(jnp.bfloat16).reshape(num_seqs * CHUNK_LEN, D_MODEL)
    gate_proj = jnp.dot(flat, w_gate, preferred_element_type=jnp.float32)
    up_proj = jnp.dot(flat, w_up, preferred_element_type=jnp.float32)
    gated = (jax.nn.gelu(gate_proj, approximate=True) * up_proj).astype(jnp.bfloat16)
    down_out = jnp.dot(gated, w_down, preferred_element_type=jnp.float32).astype(jnp.bfloat16).reshape(num_seqs, CHUNK_LEN, D_MODEL)
    return (hidden.astype(jnp.float32) + rms_norm(down_out, norm_post)).astype(jnp.bfloat16)


def reference(x, start, k_local, v_local, k_global, v_global, norms, w_q, w_k, w_v, w_o, w_gate, w_up, w_down):
    hidden, k_local_new, v_local_new = attention_half(x, start, k_local, v_local, norms[0, 0], norms[0, 1], w_q[0], w_k[0], w_v[0], w_o[0], True)
    hidden = mlp_half(hidden, norms[0, 2], norms[0, 3], w_gate[0], w_up[0], w_down[0])
    hidden, k_global_new, v_global_new = attention_half(hidden, start, k_global, v_global, norms[1, 0], norms[1, 1], w_q[1], w_k[1], w_v[1], w_o[1], False)
    hidden = mlp_half(hidden, norms[1, 2], norms[1, 3], w_gate[1], w_up[1], w_down[1])
    return (hidden, k_local_new, v_local_new, k_global_new, v_global_new)
```

```python
import jax
import jax.numpy as jnp
import numpy as np
from jax import lax
from jax.experimental import pallas as pl
from jax.experimental.pallas import tpu as pltpu
from jax.sharding import PartitionSpec as P

SOFT_CAP = 50.0
NORM_EPS = 1e-6
ROPE_BASE = 10000.0
MASKED = -1e30
DIST = 2
LOWEST = -3e38
LOG2E = 1.4426950408889634

BF16 = jnp.bfloat16
F32 = jnp.float32
MESH_ID = pl.DeviceIdType.MESH
ANY = pl.BlockSpec(memory_space=pl.ANY)
VMEM = pl.BlockSpec(memory_space=pltpu.VMEM)
SMEM = pl.BlockSpec(memory_space=pltpu.SMEM)

TILE = 256
SLOTS = 4
DOWN = 2
QROWS = 256
KEYS = 512
OUT = 512
VMEM_LIMIT = 67_000_000
ATT_PLAN = (0, 4, 6, 11, 13, 15, 17, 20, 25)
MLP_PLAN = (0, 2, 3, 5, 6, 8, 10, 12, 14)
SWAP_ORDER = (2, 1, 3, 0)
DO_COMPUTE = True
DO_COMM = True

RS_RIGHT = ((2, 0), (1, 1), (1, 0))
RS_LEFT = ((2, 1), (3, 0), (3, 1))
AG_RIGHT = ((0, 0), (0, 1), (3, 0))
AG_LEFT = ((0, 1), (0, 0), (1, 1))
AG_FROM_LEFT = ((3, 0), (3, 1), (2, 0))
AG_FROM_RIGHT = ((1, 1), (1, 0), (2, 1))


def dot(a, b):
    return jnp.dot(a, b, preferred_element_type=F32)


def dot_nt(a, b):
    return lax.dot_general(a, b, (((1,), (1,)), ((), ())), preferred_element_type=F32)


def layers_kernel(x_hbm, start_ref, freq_ref, norms_ref, kl_hbm, vl_hbm, kg_hbm, vg_hbm,
                  wq_hbm, wk_hbm, wv_hbm, wo_hbm, wg_hbm, wu_hbm, wd_hbm,
                  xo_hbm, kn_hbm, vn_hbm,
                  g, y, rb, ring_l, ring_r, xs, cos_ref, sin_ref, bias, wqkv, wo, slots, h_sc, q_sc, o_sc, kbuf, vbuf, t_sc, mx_sc,
                  s_x, s_attw, s_slot, s_kv, s_kvo, s_xo,
                  rs_ds, rs_dr, rs_rl, rs_rr, rs_sr, ag_sr, ag_rl, ag_rr, ag_ds, ag_dr):
    chunk, dim = g.shape[1], g.shape[2]
    rows = xs.shape[1]
    half = rows // 2
    piece = rows // 4
    hd = kbuf.shape[2]
    past = kbuf.shape[1] - chunk
    n_q = wq_hbm.shape[2] // TILE
    heads = wq_hbm.shape[2] // hd
    ffn = wg_hbm.shape[2]
    n_up = ffn // TILE
    n_down = dim // TILE
    per_phase = 2 * n_up + n_down
    n_tiles = 4 * per_phase
    n_blocks = heads * chunk // QROWS
    per_head = chunk // QROWS
    c1 = (hd ** -0.5) / SOFT_CAP
    c2 = SOFT_CAP * LOG2E

    dp = lax.axis_index('dp')
    me = lax.axis_index('tp')
    chip = me // 2
    core = me % 2
    right = (dp, ((chip + 1) % 4) * 2 + core)
    left = (dp, ((chip + 3) % 4) * 2 + core)
    sibling = (dp, chip * 2 + 1 - core)

    def base(offset, c):
        return ((chip + offset) % 4 * 2 + c) * rows

    def span(start, size):
        return pl.ds(pl.multiple_of(start, 16), size)

    def push(src, dst, ssem, rsem, dev):
        return pltpu.make_async_remote_copy(src_ref=src, dst_ref=dst, send_sem=ssem, recv_sem=rsem, device_id=dev, device_id_type=MESH_ID)

    def att_weight_copies(l):
        out = [pltpu.make_async_copy(wq_hbm.at[l, :, pl.ds(i * TILE, TILE)], wqkv.at[i], s_attw.at[i]) for i in range(n_q)]
        out.append(pltpu.make_async_copy(wk_hbm.at[l], wqkv.at[n_q, :, pl.ds(0, hd)], s_attw.at[n_q]))
        out.append(pltpu.make_async_copy(wv_hbm.at[l], wqkv.at[n_q, :, pl.ds(hd, hd)], s_attw.at[n_q + 1]))
        out.append(pltpu.make_async_copy(wo_hbm.at[l], wo, s_attw.at[n_q + 2]))
        return out

    def cache_copies(k_hbm, v_hbm, s):
        return [pltpu.make_async_copy(k_hbm.at[s, pl.ds(0, past)], kbuf.at[s, pl.ds(0, past)], s_kv.at[s, 0]),
                pltpu.make_async_copy(v_hbm.at[s, pl.ds(0, past)], vbuf.at[s, pl.ds(0, past)], s_kv.at[s, 1])]

    def start_tile(m):
        layer = m // (2 * per_phase)
        j = m % per_phase
        slot = m % SLOTS

        @pl.when((j < 2 * n_up) & (j % 2 == 0))
        def _():
            pltpu.make_async_copy(wg_hbm.at[layer, :, pl.ds(pl.multiple_of(j // 2 * TILE, TILE), TILE)], slots.at[slot], s_slot.at[slot]).start()

        @pl.when((j < 2 * n_up) & (j % 2 == 1))
        def _():
            pltpu.make_async_copy(wu_hbm.at[layer, :, pl.ds(pl.multiple_of(j // 2 * TILE, TILE), TILE)], slots.at[slot], s_slot.at[slot]).start()

        @pl.when(j >= 2 * n_up)
        def _():
            pltpu.make_async_copy(wd_hbm.at[layer, :, pl.ds(pl.multiple_of((j - 2 * n_up) * TILE, TILE), TILE)],
                                  slots.at[slot, pl.ds(0, ffn)], s_slot.at[slot]).start()

    def next_tile(m):
        @pl.when(m + SLOTS < n_tiles)
        def _():
            start_tile(m + SLOTS)

    def wait_up_tile(slot):
        pltpu.make_async_copy(wg_hbm.at[0, :, pl.ds(0, TILE)], slots.at[slot], s_slot.at[slot]).wait()

    def wait_down_tile(slot):
        pltpu.make_async_copy(wd_hbm.at[0, :, pl.ds(0, TILE)], slots.at[slot, pl.ds(0, ffn)], s_slot.at[slot]).wait()

    def swap(s, r, cols):
        return push(y.at[s, span(base(r, 1 - core), rows), cols], rb.at[s, r, :, cols], rs_ds.at[s, r], rs_dr.at[s, r], sibling)

    def swap_columns(s, first, size):
        if DO_COMM:
            for r in SWAP_ORDER:
                swap(s, r, pl.ds(pl.multiple_of(first, TILE), size)).start()

    def swapped(s, r):
        return swap(s, r, pl.ds(0, dim))

    def rs_right(s, u, k):
        r, hh = RS_RIGHT[k]
        src = y.at[s, span(base(r, core) + u * half + hh * piece, piece)]
        return push(src, ring_l.at[s, u, k], rs_sr.at[s, u, 0, k], rs_rl.at[s, u, k], right)

    def rs_left(s, u, k):
        r, hh = RS_LEFT[k]
        src = y.at[s, span(base(r, core) + u * half + hh * piece, piece)]
        return push(src, ring_r.at[s, u, k], rs_sr.at[s, u, 1, k], rs_rr.at[s, u, k], left)

    def add_in(s, row0, n, src):
        step = min(1024, dim)

        def body(i, carry):
            cols = pl.ds(pl.multiple_of(i * step, step), step)
            total = y[s, span(row0, n), cols].astype(F32) + src[:, cols].astype(F32)
            y[s, span(row0, n), cols] = total.astype(BF16)
            return carry

        lax.fori_loop(0, dim // step, body, 0)

    def fold(s, u, r):
        if u == 0:
            swapped(s, r).wait_recv()
        add_in(s, base(r, core) + u * half, half, rb.at[s, r, span(u * half, half)])

    def rs1(s, u):
        fold(s, u, 2)
        rs_right(s, u, 0).start()
        rs_left(s, u, 0).start()

    def rs2(s, u):
        fold(s, u, 1)
        rs_right(s, u, 1).start()
        fold(s, u, 3)
        rs_left(s, u, 1).start()

    def rs3(s, u):
        rs_right(s, u, 0).wait_recv()
        add_in(s, base(1, core) + u * half, piece, ring_l.at[s, u, 0])
        rs_right(s, u, 2).start()
        rs_left(s, u, 0).wait_recv()
        add_in(s, base(3, core) + u * half + piece, piece, ring_r.at[s, u, 0])
        rs_left(s, u, 2).start()

    def rs4_wait(s, u):
        if u == 0:
            swapped(s, 0).wait_recv()
        for k in (1, 2):
            rs_right(s, u, k).wait_recv()
            rs_left(s, u, k).wait_recv()

    def rs_drain(s):
        for r in range(4):
            swapped(s, r).wait_send()
        for u in range(2):
            for k in range(3):
                rs_right(s, u, k).wait_send()
                rs_left(s, u, k).wait_send()

    def norm_row(i):
        return norms_ref[i // 4, pl.ds(i % 4, 1)]

    def inv_rms(v):
        return lax.rsqrt(jnp.sum(v * v, axis=-1, keepdims=True) * (1.0 / dim) + NORM_EPS)

    def finish(s, u, post, has_next):
        def body(hh, carry):
            row0 = u * half + hh * piece
            loc = span(row0, piece)
            total = (y[s, span(base(0, core) + row0, piece)].astype(F32) + rb[s, 0, loc].astype(F32)
                     + ring_l[s, u, 2 - hh].astype(F32) + ring_r[s, u, 1 + hh].astype(F32))
            v = total.astype(BF16).astype(F32)
            x1 = (xs[s, loc].astype(F32) + v * inv_rms(v) * (1.0 + norm_row(post))).astype(BF16)
            xs[s, loc] = x1
            if has_next:
                w = x1.astype(F32)
                a = w * inv_rms(w) * (1.0 + norm_row(post + 1))
                g[s, span(base(0, core) + row0, piece)] = a.astype(BF16)
            return carry

        lax.fori_loop(0, 2, body, 0)

    def ag_piece(t, u, where):
        r, hh = where
        return g.at[t, span(base(r, core) + u * half + hh * piece, piece)]

    def ag_right(t, u, k, table=AG_RIGHT):
        ref = ag_piece(t, u, table[k])
        return push(ref, ref, ag_sr.at[t, u, 0, k], ag_rl.at[t, u, k], right)

    def ag_left(t, u, k, table=AG_LEFT):
        ref = ag_piece(t, u, table[k])
        return push(ref, ref, ag_sr.at[t, u, 1, k], ag_rr.at[t, u, k], left)

    def from_left(t, u, k):
        ag_right(t, u, k, AG_FROM_LEFT).wait_recv()

    def from_right(t, u, k):
        ag_left(t, u, k, AG_FROM_RIGHT).wait_recv()

    def ag_d2d(t, u, r):
        ref = g.at[t, span(base(r, core) + u * half, half)]
        return push(ref, ref, ag_ds.at[t, u, r], ag_dr.at[t, u, r], sibling)

    def ag1(t, u):
        for k in range(2):
            ag_right(t, u, k).start()
            ag_left(t, u, k).start()
        ag_d2d(t, u, 0).start()

    def ag2(t, u):
        from_left(t, u, 0)
        ag_right(t, u, 2).start()
        from_right(t, u, 0)
        ag_left(t, u, 2).start()

    def ag3(t, u):
        from_left(t, u, 1)
        ag_d2d(t, u, 3).start()
        from_right(t, u, 1)
        ag_d2d(t, u, 1).start()

    def ag4(t, u):
        from_left(t, u, 2)
        from_right(t, u, 2)
        ag_d2d(t, u, 2).start()

    def ag5(t):
        for u in range(2):
            for r in range(4):
                ref = g.at[t, span(base(r, 1 - core) + u * half, half)]
                push(ref, ref, ag_ds.at[t, u, r], ag_dr.at[t, u, r], sibling).wait_recv()

    def ag_drain(t):
        for u in range(2):
            for k in range(3):
                ag_right(t, u, k).wait_send()
                ag_left(t, u, k).wait_send()
            for r in range(4):
                ag_d2d(t, u, r).wait_send()

    def rope(v, s):
        return v * cos_ref[s] + pltpu.roll(v, hd // 2, 1) * sin_ref[s]

    def project_q(i, s):
        p = dot(g[s], wqkv[i])
        for hh in range(TILE // hd):
            rot = rope(p[:, hh * hd:(hh + 1) * hd], s).astype(BF16)
            for b in range(per_head):
                q_sc[(i * (TILE // hd) + hh) * per_head + b] = rot[b * QROWS:(b + 1) * QROWS]

    def project_kv(s):
        p = dot(g[s], wqkv[n_q])
        kbuf[s, pl.ds(past, chunk)] = rope(p[:, :hd], s).astype(BF16)
        vbuf[s, pl.ds(past, chunk)] = p[:, hd:].astype(BF16)

    def fresh_out(s, l):
        return [pltpu.make_async_copy(kbuf.at[s, pl.ds(past, chunk)], kn_hbm.at[l, s], s_kvo.at[0]),
                pltpu.make_async_copy(vbuf.at[s, pl.ds(past, chunk)], vn_hbm.at[l, s], s_kvo.at[1])]

    def scores(b, s, l):
        tok = (b % per_head) * QROWS
        diff = lax.broadcasted_iota(jnp.int32, (QROWS, KEYS), 1) - lax.broadcasted_iota(jnp.int32, (QROWS, KEYS), 0)
        oldest = jnp.where(l == 0, start_ref[s] - past, -past) + tok
        q = q_sc[b]
        top = None
        for kb in range((past + chunk) // KEYS):
            first = kb * KEYS
            cols = pl.ds(first, KEYS)
            t = jnp.tanh(dot_nt(q, kbuf[s, cols]) * c1)
            if past // 2 <= first < past:
                t = t + bias[s, :, cols]
            if first < chunk:
                t = jnp.where(diff > oldest - first, t, MASKED)
            if first >= past:
                t = jnp.where(diff <= tok - (first - past), t, MASKED)
            t_sc[:, cols] = t
            for i in range(KEYS // hd):
                ti = t[:, i * hd:(i + 1) * hd]
                top = ti if top is None else jnp.maximum(top, ti)
        mx_sc[...] = top

    def weigh(b, s):
        mc = jnp.max(mx_sc[...], axis=-1, keepdims=True) * c2
        mc = jnp.broadcast_to(mc, (QROWS, hd))
        n_kb = (past + chunk) // KEYS
        total = acc = None
        pvs = []
        for kb in range(n_kb):
            cols = pl.ds(kb * KEYS, KEYS)
            if kb >= DIST:
                mc = jnp.maximum(mc, jnp.minimum(pvs[kb - DIST], LOWEST))
            ps = []
            for i in range(KEYS // hd):
                pi = jnp.exp2(t_sc[:, pl.ds(kb * KEYS + i * hd, hd)] * c2 - mc)
                total = pi if total is None else total + pi
                ps.append(pi.astype(BF16))
            pv = dot(jnp.concatenate(ps, axis=1), vbuf[s, cols])
            pvs.append(pv)
            acc = pv if acc is None else acc + pv
        o = acc / jnp.sum(total, axis=-1, keepdims=True)
        o_sc[pl.ds(pl.multiple_of((b % per_head) * QROWS, QROWS), QROWS), pl.ds(pl.multiple_of(b // per_head * hd, hd), hd)] = o.astype(BF16)

    def out_tile(i, s):
        step = min(OUT, dim)
        cols = pl.ds(pl.multiple_of(i * step, step), step)
        y[s, :, cols] = dot(o_sc[...], wo[:, cols]).astype(BF16)

    def up_tile(jj, s, m0):
        m = m0 + 2 * jj
        sa, sb = m % SLOTS, (m + 1) % SLOTS
        wait_up_tile(sa)
        wait_up_tile(sb)
        gate = dot(g[s], slots[sa])
        up = dot(g[s], slots[sb])
        h_sc[:, pl.ds(pl.multiple_of(jj * TILE, TILE), TILE)] = (jax.nn.gelu(gate, approximate=True) * up).astype(BF16)
        next_tile(m)
        next_tile(m + 1)

    def down_tiles(n, s, m0):
        m = m0 + 2 * n_up + DOWN * n
        for i in range(DOWN):
            wait_down_tile((m + i) % SLOTS)
        for i in range(DOWN):
            cols = pl.ds(pl.multiple_of((DOWN * n + i) * TILE, TILE), TILE)
            y[s, :, cols] = dot(h_sc[...], slots[(m + i) % SLOTS, pl.ds(0, ffn)]).astype(BF16)
        for i in range(DOWN):
            next_tile(m + i)

    def events(t, post, reduce, gather):
        def reduced(u):
            @pl.when(reduce)
            def _():
                rs4_wait(t, u)

                @pl.when(gather)
                def _():
                    finish(t, u, post, True)
                    ag1(t, u)

                @pl.when(jnp.logical_not(gather))
                def _():
                    finish(t, u, post, False)

        def if_reduce(*what):
            def run():
                @pl.when(reduce)
                def _():
                    for f, u in what:
                        f(t, u)
            return run

        def if_gather(f, u):
            return lambda: pl.when(gather)(lambda: f(t, u))

        return (if_reduce((rs3, 0), (rs2, 1)), if_reduce((rs3, 1)), lambda: reduced(0), lambda: reduced(1),
                if_gather(ag2, 0), if_gather(ag3, 0), if_gather(ag2, 1), if_gather(ag3, 1), if_gather(ag4, 0))

    def at(step, low, high, plan, todo):
        if DO_COMM:
            for when, what in zip(plan, todo):
                if low <= when < high:
                    pl.when(step == when)(what)

    def tail(s, t, plan, todo, last, reduce, gather):
        if DO_COMM:
            for when, what in zip(plan, todo):
                if when >= last:
                    what()
            for u in range(2):
                rs1(s, u)
                if u == 0:
                    rs2(s, u)

            @pl.when(gather)
            def _():
                ag4(t, 1)
                ag5(t)
                ag_drain(t)
            pl.when(reduce)(lambda: rs_drain(t))

    def att_phase(l, s):
        t = 1 - s
        reduce = (l > 0) | (s > 0)
        todo = events(t, 4 * l - 1 + 2 * s, reduce, l >= 0)
        step = min(OUT, dim)
        first_block = n_q + 1
        first_out = first_block + 2 * n_blocks
        last = first_out + dim // step
        plan = ATT_PLAN
        if DO_COMPUTE:
            for c in att_weight_copies(l)[:-1]:
                pl.when(s == 0)(c.wait)

        def proj(i, carry):
            if DO_COMPUTE:
                project_q(i, s)
            at(i, 0, n_q, plan, todo)
            return carry

        lax.fori_loop(0, n_q, proj, 0)
        if DO_COMPUTE:
            project_kv(s)
            for c in fresh_out(s, l):
                c.start()
            for c in cache_copies(kl_hbm, vl_hbm, s):
                c.wait()
        at(n_q, n_q, first_block, plan, todo)

        def blk(i, carry):
            if DO_COMPUTE:
                pl.when(i % 2 == 0)(lambda: scores(i // 2, s, l))
                pl.when(i % 2 == 1)(lambda: weigh(i // 2, s))
            at(first_block + i, first_block, first_out, plan, todo)
            return carry

        lax.fori_loop(0, 2 * n_blocks, blk, 0)
        if DO_COMPUTE:
            @pl.when(l == 0)
            def _():
                for c in cache_copies(kg_hbm, vg_hbm, s):
                    c.start()
            pl.when(s == 0)(att_weight_copies(l)[-1].wait)

        def out_body(i, carry):
            if DO_COMPUTE:
                out_tile(i, s)
            swap_columns(s, i * step, step)
            at(first_out + i, first_out, last, plan, todo)
            return carry

        lax.fori_loop(0, dim // step, out_body, 0)
        if DO_COMPUTE:
            @pl.when((s == 1) & (l == 0))
            def _():
                for c in att_weight_copies(1):
                    c.start()
            for c in fresh_out(s, l):
                c.wait()
        tail(s, t, plan, todo, last, reduce, l >= 0)

    def mlp_phase(l, s):
        t = 1 - s
        m0 = (2 * l + s) * per_phase
        gather = (l == 0) | (s == 0)
        todo = events(t, 4 * l + 1 + 2 * s, l >= 0, gather)
        last = n_up + n_down // DOWN
        plan = MLP_PLAN

        def ups(jj, carry):
            if DO_COMPUTE:
                up_tile(jj, s, m0)
            at(jj, 0, n_up, plan, todo)
            return carry

        lax.fori_loop(0, n_up, ups, 0)

        def downs(n, carry):
            if DO_COMPUTE:
                down_tiles(n, s, m0)
            swap_columns(s, n * (DOWN * TILE), DOWN * TILE)
            at(n_up + n, n_up, last, plan, todo)
            return carry

        lax.fori_loop(0, last - n_up, downs, 0)
        tail(s, t, plan, todo, last, l >= 0, gather)

    xcopy = pltpu.make_async_copy(x_hbm, xs, s_x)
    xcopy.start()
    barrier = pltpu.get_barrier_semaphore()
    for dev in (sibling, left, right):
        pl.semaphore_signal(barrier, inc=1, device_id=dev, device_id_type=MESH_ID)

    def first_norm(s):
        def body(k, carry):
            v = xs[s, span(k * piece, piece)].astype(F32)
            a = v * inv_rms(v) * (1.0 + norm_row(0))
            g[s, span(base(0, core) + k * piece, piece)] = a.astype(BF16)
            return carry

        lax.fori_loop(0, 4, body, 0)

    xcopy.wait()
    first_norm(0)
    pl.semaphore_wait(barrier, 3)
    if DO_COMM:
        for u in range(2):
            ag1(0, u)
    if DO_COMPUTE:
        for c in att_weight_copies(0):
            c.start()
        for s in range(2):
            for c in cache_copies(kl_hbm, vl_hbm, s):
                c.start()
        for m in range(SLOTS):
            start_tile(jnp.int32(m))
    first_norm(1)
    for s in range(2):
        pos = (lax.broadcasted_iota(jnp.int32, (chunk, hd), 0) + start_ref[s]).astype(F32)
        angle = pos * freq_ref[...]
        low = lax.broadcasted_iota(jnp.int32, (chunk, hd), 1) < hd // 2
        cos_ref[s] = jnp.cos(angle)
        sin = jnp.sin(angle)
        sin_ref[s] = jnp.where(low, -sin, sin)
        bias[s] = jnp.where(lax.broadcasted_iota(jnp.int32, (1, past), 1) < start_ref[s], 0.0, MASKED)
    if DO_COMM:
        for u in range(2):
            ag2(0, u)
        for u in range(2):
            ag1(1, u)
        for u in range(2):
            ag3(0, u)
        for u in range(2):
            ag4(0, u)
        ag5(0)
        ag_drain(0)

    def layer(l, carry):
        def att(s, carry):
            att_phase(l, s)
            return carry

        def mlp(s, carry):
            mlp_phase(l, s)
            return carry

        lax.fori_loop(0, 2, att, 0)
        lax.fori_loop(0, 2, mlp, 0)
        return carry

    lax.fori_loop(0, 2, layer, 0)

    out0 = pltpu.make_async_copy(xs.at[0], xo_hbm.at[0], s_xo.at[0])
    out0.start()
    if DO_COMM:
        rs3(1, 0)
        rs2(1, 1)
        rs3(1, 1)

        for u in range(2):
            rs4_wait(1, u)
            finish(1, u, 7, False)
        rs_drain(1)
    out1 = pltpu.make_async_copy(xs.at[1], xo_hbm.at[1], s_xo.at[1])
    out1.start()
    out0.wait()
    out1.wait()


def run_layers(x, start, freq, norms, kl, vl, kg, vg, wq, wk, wv, wo, wg, wu, wd):
    seqs, rows, dim = x.shape
    past, hd = kl.shape[1], kl.shape[2]
    chunk = kg.shape[1] - past
    n_q = wq.shape[2] // TILE
    ring = pltpu.VMEM((2, 2, 3, rows // 4, dim), BF16)
    keys = pltpu.VMEM((2, past + chunk, hd), BF16)
    whole = pltpu.VMEM((2, chunk, dim), BF16)
    table = pltpu.VMEM((2, chunk, hd), F32)

    def dmas(*shape):
        return pltpu.SemaphoreType.DMA(shape)

    scratch = [
        whole, whole,
        pltpu.VMEM((2, 4, rows, dim), BF16),
        ring, ring,
        pltpu.VMEM((2, rows, dim), BF16),
        table, table,
        pltpu.VMEM((2, 1, past), F32),
        pltpu.VMEM((n_q + 1, dim, TILE), BF16),
        pltpu.VMEM(wo.shape[1:], BF16),
        pltpu.VMEM((SLOTS, max(dim, wd.shape[1]), TILE), BF16),
        pltpu.VMEM((chunk, wg.shape[2]), BF16),
        pltpu.VMEM((wq.shape[2] // hd * chunk // QROWS, QROWS, hd), BF16),
        pltpu.VMEM((chunk, wq.shape[2]), BF16),
        keys, keys,
        pltpu.VMEM((QROWS, past + chunk), F32),
        pltpu.VMEM((QROWS, hd), F32),
        pltpu.SemaphoreType.DMA, dmas(n_q + 3), dmas(SLOTS), dmas(2, 2), dmas(2), dmas(2),
    ]
    chips = [dmas(2, 2, 3)] * 2
    cores = [dmas(2, 2, 4)] * 2
    swaps = [dmas(2, 4)] * 2
    sends = [dmas(2, 2, 2, 3)]
    scratch += swaps + chips + sends + sends + chips + cores
    return pl.pallas_call(
        layers_kernel,
        out_shape=(jax.ShapeDtypeStruct(x.shape, BF16),) + (jax.ShapeDtypeStruct((2, seqs, chunk, hd), BF16),) * 2,
        in_specs=[ANY, SMEM, VMEM, VMEM] + [ANY] * 11,
        out_specs=(ANY,) * 3,
        scratch_shapes=scratch,
        compiler_params=pltpu.CompilerParams(collective_id=0, has_side_effects=True, vmem_limit_bytes=VMEM_LIMIT),
        name='layers',
    )(x, start, freq, norms, kl, vl, kg, vg, wq, wk, wv, wo, wg, wu, wd)


def cache_kernel(start_ref, x, k_new, v_new, kl, vl, kg, vg, x_o, kl_o, vl_o, kg_o, vg_o, xbuf, buf, fresh, s_x, s_in, s_fr, s_out):
    chunk = k_new.shape[2]
    window = kl.shape[1]
    lead = fresh.shape[1] - chunk
    n_buf = buf.shape[0]
    jobs = []
    for b in range(kl.shape[0]):
        for l, pairs in enumerate((((kl, k_new, kl_o), (vl, v_new, vl_o)), ((kg, k_new, kg_o), (vg, v_new, vg_o)))):
            jobs += [(src, new, dst, l, b) for src, new, dst in pairs]

    def load(i):
        src, new, _, l, b = jobs[i]
        k = i % n_buf
        return (pltpu.make_async_copy(src.at[b], buf.at[k, pl.ds(0, src.shape[1])], s_in.at[k]),
                pltpu.make_async_copy(new.at[l, b], fresh.at[k, pl.ds(0, chunk)], s_fr.at[k]))

    def store(i):
        src, _, dst, _, b = jobs[i]
        k = i % n_buf
        return pltpu.make_async_copy(buf.at[k, pl.ds(0, src.shape[1])], dst.at[b], s_out.at[k])

    x_in = pltpu.make_async_copy(x, xbuf, s_x)
    x_out = pltpu.make_async_copy(xbuf, x_o, s_x)
    x_in.start()
    for i in range(n_buf):
        for c in load(i):
            c.start()
    x_in.wait()
    x_out.start()
    for i, (_, _, _, l, b) in enumerate(jobs):
        k = i % n_buf
        for c in load(i):
            c.wait()
        start = start_ref[b]
        r = start % lead
        at = pl.multiple_of(start - r, lead)
        rolled = pltpu.roll(fresh[k].astype(F32), r, 0)
        row = lax.broadcasted_iota(jnp.int32, rolled.shape, 0)
        old = buf[k, pl.ds(at, chunk + lead)].astype(F32)
        buf[k, pl.ds(at, chunk + lead)] = jnp.where((row >= r) & (row < r + chunk), rolled, old).astype(BF16)
        if l == 0:
            over = buf[k, pl.ds(window, chunk)].astype(F32)
            row = lax.broadcasted_iota(jnp.int32, over.shape, 0)
            head = buf[k, pl.ds(0, chunk)].astype(F32)
            buf[k, pl.ds(0, chunk)] = jnp.where(row < start + chunk - window, over, head).astype(BF16)
        store(i).start()
        if i >= 1 and i - 1 + n_buf < len(jobs):
            store(i - 1).wait()
            for c in load(i - 1 + n_buf):
                c.start()
    for i in range(max(0, len(jobs) - n_buf), len(jobs)):
        store(i).wait()
    x_out.wait()


def write_caches(start, x, k_new, v_new, kl, vl, kg, vg):
    hd = kl.shape[2]
    chunk = k_new.shape[2]
    lead = 16
    depth = max(kl.shape[1] + chunk, kg.shape[1]) + lead
    n_buf = 8
    dmas = pltpu.SemaphoreType.DMA((n_buf,))
    return pl.pallas_call(
        cache_kernel,
        out_shape=tuple(jax.ShapeDtypeStruct(c.shape, BF16) for c in (x, kl, vl, kg, vg)),
        in_specs=[SMEM] + [ANY] * 7,
        out_specs=(ANY,) * 5,
        scratch_shapes=[pltpu.VMEM(x.shape, BF16), pltpu.VMEM((n_buf, depth, hd), BF16), pltpu.VMEM((n_buf, chunk + lead, hd), BF16),
                        pltpu.SemaphoreType.DMA, dmas, dmas, dmas],
        compiler_params=pltpu.CompilerParams(vmem_limit_bytes=VMEM_LIMIT),
        name='write_caches',
    )(start, x, k_new, v_new, kl, vl, kg, vg)


def solution(mesh):
    act_spec = P('dp', 'tp', None)
    cache_spec = P('dp', None, 'tp', None)
    col_spec = P(None, None, 'tp')
    row_spec = P(None, 'tp', None)
    arg_specs = (act_spec, P('dp'), cache_spec, cache_spec, cache_spec, cache_spec, P(), col_spec, col_spec, col_spec, row_spec, col_spec, col_spec, row_spec)
    result_specs = (act_spec, cache_spec, cache_spec, cache_spec, cache_spec)

    def device_step(x, start, k_local, v_local, k_global, v_global, norms, w_q, w_k, w_v, w_o, w_gate, w_up, w_down):
        hd = k_local.shape[3]
        freq = ROPE_BASE ** (np.arange(hd // 2) * (-2.0 / hd))
        freq = jnp.asarray(np.concatenate([freq, freq])[None], F32)
        flat = [c.reshape(c.shape[0], c.shape[1], hd) for c in (k_local, v_local, k_global, v_global)]
        x_out, k_new, v_new = run_layers(x, start, freq, norms, *flat, w_q, w_k, w_v, w_o, w_gate, w_up, w_down)
        x_out, *caches = write_caches(start, x_out, k_new, v_new, *flat)
        return (x_out,) + tuple(c.reshape(c.shape[0], c.shape[1], 1, hd) for c in caches)

    return jax.shard_map(device_step, mesh=mesh, in_specs=arg_specs, out_specs=result_specs, check_vma=False)
```

```python
import jax
import jax.numpy as jnp
import numpy as np
from jax import lax
from jax.experimental import pallas as pl
from jax.experimental.pallas import tpu as pltpu
from jax.sharding import PartitionSpec as P

SOFT_CAP = 50.0
NORM_EPS = 1e-6
ROPE_BASE = 10000.0
MASKED = -1e30
DIST = 2
LOWEST = -3e38
LOG2E = 1.4426950408889634

BF16 = jnp.bfloat16
F32 = jnp.float32
MESH_ID = pl.DeviceIdType.MESH
ANY = pl.BlockSpec(memory_space=pl.ANY)
VMEM = pl.BlockSpec(memory_space=pltpu.VMEM)
SMEM = pl.BlockSpec(memory_space=pltpu.SMEM)

TILE = 256
SLOTS = 5
DOWN = 2
QROWS = 256
KEYS = 512
OUT = 2048
VMEM_LIMIT = 67_000_000
LAYERS_LIMIT = 67_000_000
SWAP = 1024
ATT_PLAN = (4, 10, 12, 16, 19, 21, 22, 23, 24)
MLP_PLAN = (2, 5, 6, 8, 10, 11, 13, 15, 16)
LAST_RS3 = 7
SWAP_ORDER = (2, 1, 3, 0)
DO_COMPUTE = True
DO_COMM = True

PAIR = range(2)

RS_RIGHT = ((2, 0), (1, 1), (1, 0))
RS_LEFT = ((2, 1), (3, 0), (3, 1))
AG_RIGHT = ((0, 0), (0, 1), (3, 0))
AG_LEFT = ((0, 1), (0, 0), (1, 1))
AG_FROM_LEFT = ((3, 0), (3, 1), (2, 0))
AG_FROM_RIGHT = ((1, 1), (1, 0), (2, 1))


def repeat(n, body, low=0):
    lax.fori_loop(low, n, body, 0)


def dot(a, b):
    return jnp.dot(a, b, preferred_element_type=F32)


def dot_nt(a, b):
    return lax.dot_general(a, b, (((1,), (1,)), ((), ())), preferred_element_type=F32)


def layers_kernel(x_hbm, start_ref, freq_ref, norms_ref, kl_hbm, vl_hbm, kg_hbm, vg_hbm,
                  wq_hbm, wk_hbm, wv_hbm, wo_hbm, wg_hbm, wu_hbm, wd_hbm,
                  xo_hbm, kn_hbm, vn_hbm,
                  g, y, rb, ring_l, ring_r, xs, cos_ref, sin_ref, bias, wqkv, wo, slots, h_sc, q_sc, o_sc, kbuf, vbuf, t_sc, mx_sc,
                  s_x, s_attw, s_slot, s_kv, s_kvo, s_xo, credit,
                  rs_ds, rs_dr, rs_rl, rs_rr, rs_sr, ag_sr, ag_rl, ag_rr, ag_ds, ag_dr):
    devices, half, dim = g.shape[1], g.shape[3], g.shape[4]
    chunk = devices * 2 * half
    piece = half // 2
    hd = kbuf.shape[1]
    past = kbuf.shape[0] - chunk
    n_q = wq_hbm.shape[2] // TILE
    heads = wq_hbm.shape[2] // hd
    ffn = wg_hbm.shape[2]
    n_up = ffn // TILE
    n_down = dim // TILE
    n_pairs = n_down // DOWN
    per_phase = 2 * n_up + n_pairs
    n_tiles = 4 * per_phase + n_pairs
    n_blocks = heads * chunk // QROWS
    per_head = chunk // QROWS
    owners = devices // per_head
    c1 = (hd ** -0.5) / SOFT_CAP
    c2 = SOFT_CAP * LOG2E

    dp = lax.axis_index('dp')
    me = lax.axis_index('tp')
    chip = me // 2
    core = me % 2
    chips = devices // 2
    right = (dp, (chip + 1) % chips * 2 + core)
    left = (dp, (chip + chips - 1) % chips * 2 + core)
    sibling = (dp, chip * 2 + 1 - core)
    partners = (sibling, left, right)

    def owner(offset, c):
        return (chip + offset) % chips * 2 + c

    def columns(first, size):
        return pl.ds(pl.multiple_of(first, TILE), size)

    def rows(hh):
        return pl.ds(pl.multiple_of(hh * piece, piece), piece)

    def push(src, dst, ssem, rsem, dev):
        return pltpu.make_async_remote_copy(src_ref=src, dst_ref=dst, send_sem=ssem, recv_sem=rsem, device_id=dev, device_id_type=MESH_ID)

    def att_weight_copies(l):
        out = [pltpu.make_async_copy(wq_hbm.at[l, :, pl.ds(i * TILE, TILE)], wqkv.at[i], s_attw.at[i]) for i in range(n_q)]
        out.append(pltpu.make_async_copy(wk_hbm.at[l], wqkv.at[n_q, :, pl.ds(0, hd)], s_attw.at[n_q]))
        out.append(pltpu.make_async_copy(wv_hbm.at[l], wqkv.at[n_q, :, pl.ds(hd, hd)], s_attw.at[n_q + 1]))
        out.append(pltpu.make_async_copy(wo_hbm.at[l], wo, s_attw.at[n_q + 2]))
        return out

    def cache_copies(k_hbm, v_hbm, s):
        return [pltpu.make_async_copy(c.at[s, pl.ds(0, past)], buf.at[pl.ds(0, past)], s_kv.at[i])
                for i, (c, buf) in enumerate(((k_hbm, kbuf), (v_hbm, vbuf)))]

    def start_tile(m):
        slot = m % SLOTS
        m = jnp.where(m < n_tiles - n_pairs, m, m - n_pairs)
        layer = m // (2 * per_phase)
        j = m % per_phase

        @pl.when((j < 2 * n_up) & (j % 2 == 0))
        def _():
            pltpu.make_async_copy(wg_hbm.at[layer, :, columns(j // 2 * TILE, TILE)], slots.at[slot, pl.ds(0, dim)], s_slot.at[slot, 0]).start()

        @pl.when((j < 2 * n_up) & (j % 2 == 1))
        def _():
            pltpu.make_async_copy(wu_hbm.at[layer, :, columns(j // 2 * TILE, TILE)], slots.at[slot, pl.ds(0, dim)], s_slot.at[slot, 0]).start()

        @pl.when(j >= 2 * n_up)
        def _():
            for i in range(DOWN):
                pltpu.make_async_copy(wd_hbm.at[layer, :, columns(((j - 2 * n_up) * DOWN + i) * TILE, TILE)],
                                      slots.at[slot, pl.ds(i * ffn, ffn)], s_slot.at[slot, i]).start()

    def next_tile(m):
        @pl.when(m + SLOTS < n_tiles)
        def _():
            start_tile(m + SLOTS)

    def wait_up_tile(slot):
        pltpu.make_async_copy(wg_hbm.at[0, :, pl.ds(0, TILE)], slots.at[slot, pl.ds(0, dim)], s_slot.at[slot, 0]).wait()

    def wait_down_pair(slot):
        for i in range(DOWN):
            pltpu.make_async_copy(wd_hbm.at[0, :, pl.ds(0, TILE)], slots.at[slot, pl.ds(i * ffn, ffn)], s_slot.at[slot, i]).wait()

    def swap(s, u, r, cols):
        which, i = (slice(None), 0) if u is None else (u, u)
        return push(y.at[s, owner(r, 1 - core), which, :, cols], rb.at[r, which, :, cols], rs_ds.at[s, i, r], rs_dr.at[s, i, r], sibling)

    def swap_columns(s, u, first, size):
        if DO_COMM:
            for r in SWAP_ORDER:
                swap(s, u, r, columns(first, size)).start()

    def swapped(s, u, r):
        return swap(s, u, r, pl.ds(0, dim))

    def rs_right(s, u, k):
        r, hh = RS_RIGHT[k]
        return push(y.at[s, owner(r, core), u, rows(hh)], ring_l.at[u, k], rs_sr.at[s, u, 0, k], rs_rl.at[s, u, k], right)

    def rs_left(s, u, k):
        r, hh = RS_LEFT[k]
        return push(y.at[s, owner(r, core), u, rows(hh)], ring_r.at[u, k], rs_sr.at[s, u, 1, k], rs_rr.at[s, u, k], left)

    def add_in(dst, src):
        step = min(1024, dim)

        def body(i, carry):
            cols = pl.ds(pl.multiple_of(i * step, step), step)
            dst[:, cols] = (dst[:, cols].astype(F32) + src[:, cols].astype(F32)).astype(BF16)
            return carry

        repeat(dim // step, body)

    def fold(s, u, r, apart):
        if apart:
            swapped(s, u, r).wait_recv()
        elif u == 0:
            swapped(s, None, r).wait_recv()
        add_in(y.at[s, owner(r, core), u], rb.at[r, u])

    def rs1(s, u, apart=False):
        fold(s, u, 2, apart)
        rs_right(s, u, 0).start()
        rs_left(s, u, 0).start()

    def rs2(s, u, apart=False):
        hold = apart and u == 1
        fold(s, u, 1, apart)
        if not hold:
            rs_right(s, u, 1).start()
        fold(s, u, 3, apart)
        if hold:
            rs_gone(s, u, 0)
            rs_right(s, u, 1).start()
        rs_left(s, u, 1).start()

    def rs3(s, u):
        rs_right(s, u, 0).wait_recv()
        add_in(y.at[s, owner(1, core), u, rows(0)], ring_l.at[u, 0])
        rs_right(s, u, 2).start()
        rs_left(s, u, 0).wait_recv()
        add_in(y.at[s, owner(3, core), u, rows(1)], ring_r.at[u, 0])
        rs_left(s, u, 2).start()

    def rs4_wait(s, u, apart=False):
        if apart:
            swapped(s, u, 0).wait_recv()
        elif u == 0:
            swapped(s, None, 0).wait_recv()
        for k in (1, 2):
            rs_right(s, u, k).wait_recv()
            rs_left(s, u, k).wait_recv()

    def rs_gone(s, u, k):
        rs_right(s, u, k).wait_send()
        rs_left(s, u, k).wait_send()

    def rs_drain(s, halves=(None,)):
        for u in halves:
            for r in range(4):
                swapped(s, u, r).wait_send()
        for u in PAIR:
            for k in range(3):
                if None in halves or u == 0 or k > 0:
                    rs_gone(s, u, k)

    def norm_row(i):
        return norms_ref[i // 4, pl.ds(i % 4, 1)]

    def inv_rms(v):
        return lax.rsqrt(jnp.sum(v * v, axis=-1, keepdims=True) * (1.0 / dim) + NORM_EPS)

    def finish(s, u, post, has_next):
        def body(hh, carry):
            at = rows(hh)
            total = (y[s, me, u, at].astype(F32) + rb[0, u, at].astype(F32)
                     + ring_l[u, 2 - hh].astype(F32) + ring_r[u, 1 + hh].astype(F32))
            v = total.astype(BF16).astype(F32)
            x1 = (xs[s, u, at].astype(F32) + v * inv_rms(v) * (1.0 + norm_row(post))).astype(BF16)
            xs[s, u, at] = x1
            if has_next:
                w = x1.astype(F32)
                g[s, me, u, at] = (w * inv_rms(w) * (1.0 + norm_row(post + 1))).astype(BF16)
            return carry

        repeat(2, body)

    def ag_right(t, u, k, table=AG_RIGHT):
        r, hh = table[k]
        ref = g.at[t, owner(r, core), u, rows(hh)]
        return push(ref, ref, ag_sr.at[t, u, 0, k], ag_rl.at[t, u, k], right)

    def ag_left(t, u, k, table=AG_LEFT):
        r, hh = table[k]
        ref = g.at[t, owner(r, core), u, rows(hh)]
        return push(ref, ref, ag_sr.at[t, u, 1, k], ag_rr.at[t, u, k], left)

    def from_left(t, u, k):
        ag_right(t, u, k, AG_FROM_LEFT).wait_recv()

    def from_right(t, u, k):
        ag_left(t, u, k, AG_FROM_RIGHT).wait_recv()

    def ag_d2d(t, u, r, c):
        ref = g.at[t, owner(r, c), u]
        return push(ref, ref, ag_ds.at[t, u, r], ag_dr.at[t, u, r], sibling)

    def ag_out(t, u, k):
        ag_right(t, u, k).start()
        ag_left(t, u, k).start()

    def ag_gone(t, u, k):
        ag_right(t, u, k).wait_send()
        ag_left(t, u, k).wait_send()

    def ag1(t, u):
        for k in PAIR:
            ag_out(t, u, k)
        ag_d2d(t, u, 0, core).start()

    def ag2(t, u):
        from_left(t, u, 0)
        ag_right(t, u, 2).start()
        from_right(t, u, 0)
        ag_left(t, u, 2).start()

    def ag3(t, u):
        from_left(t, u, 1)
        ag_d2d(t, u, 3, core).start()
        from_right(t, u, 1)
        ag_d2d(t, u, 1, core).start()

    def ag4(t, u):
        from_left(t, u, 2)
        from_right(t, u, 2)
        ag_d2d(t, u, 2, core).start()

    def ag_own(t):
        for u in PAIR:
            ag_d2d(t, u, 0, 1 - core).wait_recv()

    def ag5(t, u):
        for r in (1, 3, 2):
            ag_d2d(t, u, r, 1 - core).wait_recv()

    def ag_drain(t, first):
        for u in PAIR:
            pl.when(jnp.logical_not(first))(lambda: ag_gone(t, u, 0))
            for k in (1, 2):
                ag_gone(t, u, k)
            for r in range(4):
                ag_d2d(t, u, r, core).wait_send()

    def rows_of(v):
        return v.reshape(chunk // 2, v.shape[-1])

    def rope(v, s, u):
        return v * rows_of(cos_ref[s, :, u]) + pltpu.roll(v, hd // 2, 1) * rows_of(sin_ref[s, :, u])

    def project_q(i, u, s):
        p = dot(rows_of(g[s, :, u]), wqkv[i])
        for hh in range(TILE // hd):
            rot = rope(p[:, hh * hd:(hh + 1) * hd], s, u).astype(BF16)
            q_sc[i * (TILE // hd) + hh, :, u] = rot.reshape(devices, half, hd)

    def project_kv(u, s):
        p = dot(rows_of(g[s, :, u]), wqkv[n_q])
        k = rope(p[:, :hd], s, u).astype(BF16).reshape(devices, half, hd)
        v = p[:, hd:].astype(BF16).reshape(devices, half, hd)
        for j in range(devices):
            at = pl.ds(past + (2 * j + u) * half, half)
            kbuf[at] = k[j]
            vbuf[at] = v[j]

    def fresh_out(s, l):
        return [pltpu.make_async_copy(buf.at[pl.ds(past, chunk)], out.at[l, s], s_kvo.at[i])
                for i, (buf, out) in enumerate(((kbuf, kn_hbm), (vbuf, vn_hbm)))]

    def scores(b, s, l):
        tok = (b % per_head) * QROWS
        diff = lax.broadcasted_iota(jnp.int32, (QROWS, KEYS), 1) - lax.broadcasted_iota(jnp.int32, (QROWS, KEYS), 0)
        oldest = jnp.where(l == 0, start_ref[s] - past, -past) + tok
        q = q_sc[b // per_head, pl.ds(b % per_head * owners, owners)].reshape(QROWS, hd)
        top = None
        for kb in range((past + chunk) // KEYS):
            first = kb * KEYS
            cols = pl.ds(first, KEYS)
            t = jnp.tanh(dot_nt(q, kbuf[cols]) * c1)
            if past // 2 <= first < past:
                t = t + bias[s, :, cols]
            if first < chunk:
                t = jnp.where(diff > oldest - first, t, MASKED)
            if first >= past:
                t = jnp.where(diff <= tok - (first - past), t, MASKED)
            t_sc[:, cols] = t
            for i in range(KEYS // hd):
                ti = t[:, i * hd:(i + 1) * hd]
                top = ti if top is None else jnp.maximum(top, ti)
        mx_sc[...] = top

    def weigh(b, s):
        mc = jnp.max(mx_sc[...], axis=-1, keepdims=True) * c2
        mc = jnp.broadcast_to(mc, (QROWS, hd))
        n_kb = (past + chunk) // KEYS
        total = acc = None
        pvs = []
        for kb in range(n_kb):
            cols = pl.ds(kb * KEYS, KEYS)
            if kb >= DIST:
                mc = jnp.maximum(mc, jnp.minimum(pvs[kb - DIST], LOWEST))
            ps = []
            for i in range(KEYS // hd):
                pi = jnp.exp2(t_sc[:, pl.ds(kb * KEYS + i * hd, hd)] * c2 - mc)
                total = pi if total is None else total + pi
                ps.append(pi.astype(BF16))
            pv = dot(jnp.concatenate(ps, axis=1), vbuf[cols])
            pvs.append(pv)
            acc = pv if acc is None else acc + pv
        o = acc / jnp.sum(total, axis=-1, keepdims=True)
        o_sc[pl.ds(pl.multiple_of((b % per_head) * QROWS, QROWS), QROWS), pl.ds(pl.multiple_of(b // per_head * hd, hd), hd)] = o.astype(BF16)

    def out_tile(i, s):
        step = min(OUT, dim)
        cols = columns(i * step, step)
        y[s, :, :, :, cols] = dot(o_sc[...], wo[:, cols]).astype(BF16).reshape(devices, 2, half, step)

    def gated(x, sa, sb):
        return (jax.nn.gelu(dot(x, slots[sa, pl.ds(0, dim)]), approximate=True) * dot(x, slots[sb, pl.ds(0, dim)])).astype(BF16)

    def up_half(jj, u, s, m0):
        m = m0 + 2 * jj
        h_sc[:, u, :, columns(jj * TILE, TILE)] = gated(rows_of(g[s, :, u]), m % SLOTS, (m + 1) % SLOTS).reshape(devices, half, TILE)

    def up_tile(jj, s, m0):
        m = m0 + 2 * jj
        wait_up_tile(m % SLOTS)
        wait_up_tile((m + 1) % SLOTS)
        h = gated(g[s].reshape(chunk, dim), m % SLOTS, (m + 1) % SLOTS)
        h_sc[:, :, :, columns(jj * TILE, TILE)] = h.reshape(devices, 2, half, TILE)
        next_tile(m)
        next_tile(m + 1)

    def down_pair(n, s, m0, u=None):
        m = m0 + 2 * n_up + n
        slot = m % SLOTS
        wait_down_pair(slot)
        for i in range(DOWN):
            cols = columns((n % n_pairs * DOWN + i) * TILE, TILE)
            w = slots[slot, pl.ds(i * ffn, ffn)]
            if u is None:
                y[s, :, :, :, cols] = dot(h_sc[...].reshape(chunk, ffn), w).astype(BF16).reshape(devices, 2, half, TILE)
            else:
                y[s, :, u, :, cols] = dot(rows_of(h_sc[:, u]), w).astype(BF16).reshape(devices, half, TILE)
        next_tile(m)

    def events(t, post, reduce, gather):
        def reduced(u):
            @pl.when(reduce)
            def _():
                rs4_wait(t, u)

                @pl.when(gather)
                def _():
                    finish(t, u, post, True)
                    ag1(t, u)

                @pl.when(jnp.logical_not(gather))
                def _():
                    finish(t, u, post, False)

        def if_reduce(*what):
            def run():
                @pl.when(reduce)
                def _():
                    for f, u in what:
                        f(t, u)
            return run

        def if_gather(f, u):
            return lambda: pl.when(gather)(lambda: f(t, u))

        return (if_reduce((rs3, 0), (rs2, 1)), if_reduce((rs3, 1)), lambda: reduced(0), lambda: reduced(1),
                if_gather(ag2, 0), if_gather(ag3, 0), if_gather(ag2, 1), if_gather(ag3, 1), if_gather(ag4, 0))

    def at(step, low, high, plan, todo):
        if DO_COMM:
            for when, what in zip(plan, todo):
                if low <= when < high:
                    pl.when(step == when)(what)

    def leave(s):
        rs1(s, 0)
        rs2(s, 0)
        rs1(s, 1)

    def rest(plan, todo, last):
        if DO_COMM:
            for when, what in zip(plan, todo):
                if when >= last:
                    what()

    def att_phase(l, s):
        t = 1 - s
        reduce = (l > 0) | (s > 0)
        todo = events(t, 4 * l - 1 + 2 * s, reduce, l >= 0)
        step = min(OUT, dim)
        swap_step = min(SWAP, dim)
        n_proj = n_q + 1
        first_block = 2 * n_proj
        first_out = first_block + 2 * n_blocks
        last = first_out + dim // step
        plan = ATT_PLAN
        if DO_COMPUTE:
            for c in att_weight_copies(l)[:-1]:
                pl.when(s == 0)(c.wait)
        if DO_COMM:
            ag5(s, 0)

        def proj(i, carry):
            if DO_COMPUTE:
                pl.when(i % n_proj < n_q)(lambda: project_q(i % n_proj, i // n_proj, s))
                pl.when(i % n_proj == n_q)(lambda: project_kv(i // n_proj, s))
            if DO_COMM:
                pl.when(i == 0)(lambda: ag4(s, 1))

                @pl.when(i == n_proj - 1)
                def _():
                    ag5(s, 1)
                    ag_drain(s, (l == 0) & (s == 0))
            at(i, 0, first_block, plan, todo)
            return carry

        repeat(first_block, proj)
        if DO_COMPUTE:
            for c in fresh_out(s, l):
                c.start()
            for c in cache_copies(kl_hbm, vl_hbm, s):
                c.wait()

        def blk(i, carry):
            if DO_COMPUTE:
                pl.when(i % 2 == 0)(lambda: scores(i // 2, s, l))
                pl.when(i % 2 == 1)(lambda: weigh(i // 2, s))
            at(first_block + i, first_block, first_out, plan, todo)
            return carry

        repeat(2 * n_blocks, blk)
        if DO_COMPUTE:
            for c in fresh_out(s, l):
                c.wait()

            @pl.when((l == 0) & (s == 0))
            def _():
                for c in cache_copies(kl_hbm, vl_hbm, 1):
                    c.start()

            @pl.when(l + s == 1)
            def _():
                for c in cache_copies(kg_hbm, vg_hbm, l):
                    c.start()
            pl.when(s == 0)(att_weight_copies(l)[-1].wait)
        if DO_COMM:
            ag_own(t)

        def out_body(i, carry):
            if DO_COMPUTE:
                out_tile(i, s)
            for j in range(step // swap_step):
                swap_columns(s, None, i * step + j * swap_step, swap_step)
            at(first_out + i, first_out, last, plan, todo)
            return carry

        repeat(dim // step, out_body)
        if DO_COMPUTE:
            @pl.when((s == 1) & (l == 0))
            def _():
                for c in att_weight_copies(1):
                    c.start()
        if DO_COMM:
            leave(s)
        rest(plan, todo, last)
        if DO_COMM:
            pl.when(reduce)(lambda: rs_drain(t))

    def mlp_phase(l, s):
        t = 1 - s
        m0 = (2 * l + s) * per_phase
        gather = (l == 0) | (s == 0)
        todo = events(t, 4 * l + 1 + 2 * s, l >= 0, gather)
        first_down = n_up + 2
        last = first_down + n_pairs
        plan = MLP_PLAN
        if DO_COMM:
            ag5(s, 0)

        def halves(i, carry):
            if DO_COMPUTE:
                m = m0 + 2 * i

                @pl.when(i < 2)
                def _():
                    wait_up_tile(m % SLOTS)
                    wait_up_tile((m + 1) % SLOTS)
                up_half(i % 2, i // 2, s, m0)

                @pl.when(i >= 2)
                def _():
                    next_tile(m - 4)
                    next_tile(m - 3)
            if DO_COMM:
                pl.when(i == 0)(lambda: ag4(s, 1))

                @pl.when(i == 1)
                def _():
                    ag5(s, 1)
                    ag_drain(s, l < 0)
            at(i, 0, 4, plan, todo)
            return carry

        repeat(4, halves)

        def ups(jj, carry):
            if DO_COMPUTE:
                up_tile(jj, s, m0)
            at(2 + jj, 4, first_down, plan, todo)
            return carry

        repeat(n_up, ups, 2)

        swap_step = min(SWAP, dim)
        every = swap_step // (DOWN * TILE)

        @pl.when(gather)
        def _():
            def downs(n, carry):
                if DO_COMPUTE:
                    down_pair(n, s, m0)
                if DO_COMM:
                    pl.when(n == every - 1)(lambda: ag_own(t))
                pl.when(n % every == every - 1)(lambda: swap_columns(s, None, n // every * swap_step, swap_step))
                at(first_down + n, first_down, last, plan, todo)
                return carry

            repeat(n_pairs, downs)
            if DO_COMM:
                leave(s)
            rest(plan, todo, last)

        @pl.when(jnp.logical_not(gather))
        def _():
            rare = n_pairs // 2
            if DO_COMM:
                rest(plan[:4], todo, first_down)
                for dev in partners:
                    pl.semaphore_signal(credit, inc=1, device_id=dev, device_id_type=MESH_ID)
            for u in PAIR:
                def downs(n, carry):
                    if DO_COMPUTE:
                        down_pair(u * n_pairs + n, s, m0, u)
                    if DO_COMM:
                        if u == 0:
                            pl.when(n == rare - 1)(lambda: pl.semaphore_wait(credit, len(partners)))
                        pl.when(n % rare == rare - 1)(lambda: swap_columns(s, u, n // rare * (rare * DOWN * TILE), rare * DOWN * TILE))
                        if u == 1:
                            @pl.when(n == min(1, n_pairs - 1))
                            def _():
                                rs1(s, 0, True)
                                rs2(s, 0, True)
                            pl.when(n == min(LAST_RS3, n_pairs - 1))(lambda: rs3(s, 0))
                    return carry

                repeat(n_pairs, downs)
            if DO_COMM:
                rs1(s, 1, True)
                rs2(s, 1, True)
        if DO_COMM:
            rs_drain(t)

    xcopy = pltpu.make_async_copy(x_hbm, xs, s_x)
    xcopy.start()
    barrier = pltpu.get_barrier_semaphore()
    for dev in partners:
        pl.semaphore_signal(barrier, inc=1, device_id=dev, device_id_type=MESH_ID)

    def first_norm(s, u):
        def body(hh, carry):
            v = xs[s, u, rows(hh)].astype(F32)
            g[s, me, u, rows(hh)] = (v * inv_rms(v) * (1.0 + norm_row(0))).astype(BF16)
            return carry

        repeat(2, body)

    xcopy.wait()
    first_norm(0, 0)
    pl.semaphore_wait(barrier, len(partners))
    for u in PAIR:
        if u == 1:
            first_norm(0, 1)
        if DO_COMM:
            ag_out(0, u, 0)
            ag_d2d(0, u, 0, core).start()
    if DO_COMPUTE:
        for c in att_weight_copies(0) + cache_copies(kl_hbm, vl_hbm, 0):
            c.start()
        for m in range(SLOTS):
            start_tile(jnp.int32(m))
    for u in PAIR:
        first_norm(1, u)
    for s in PAIR:
        shape = cos_ref.shape[1:]
        pos = start_ref[s] + sum(n * lax.broadcasted_iota(jnp.int32, shape, i) for i, n in enumerate((2 * half, half, 1)))
        angle = pos.astype(F32) * freq_ref[...]
        cos_ref[s] = jnp.cos(angle)
        sin = jnp.sin(angle)
        sin_ref[s] = jnp.where(lax.broadcasted_iota(jnp.int32, shape, 3) < hd // 2, -sin, sin)
        bias[s] = jnp.where(lax.broadcasted_iota(jnp.int32, (1, past), 1) < start_ref[s], 0.0, MASKED)
    if DO_COMM:
        for u in PAIR:
            ag_gone(0, u, 0)
            ag_out(0, u, 1)
        for u in PAIR:
            ag2(0, u)
        for u in PAIR:
            ag3(0, u)
        ag4(0, 0)
        ag_own(0)
        for u in PAIR:
            ag1(1, u)

    def layer(l, carry):
        def att(s, carry):
            att_phase(l, s)
            return carry

        def mlp(s, carry):
            mlp_phase(l, s)
            return carry

        repeat(2, att)
        repeat(2, mlp)
        return carry

    repeat(2, layer)

    out = [pltpu.make_async_copy(xs.at[s, u], xo_hbm.at[s, u], s_xo.at[s, u]) for s in PAIR for u in PAIR]
    out[0].start()
    out[1].start()
    if DO_COMM:
        rs3(1, 1)
    for u in PAIR:
        if DO_COMM:
            rs4_wait(1, u, True)
            finish(1, u, 7, False)
        out[2 + u].start()
    if DO_COMM:
        rs_drain(1, PAIR)
    for copy in out:
        copy.wait()


def run_layers(x, start, freq, norms, kl, vl, kg, vg, wq, wk, wv, wo, wg, wu, wd):
    seqs, _, half, dim = x.shape
    past, hd = kl.shape[1], kl.shape[2]
    chunk = kg.shape[1] - past
    n_q = wq.shape[2] // TILE
    devices = chunk // (2 * half)
    ring = pltpu.VMEM((2, 3, half // 2, dim), BF16)
    keys = pltpu.VMEM((past + chunk, hd), BF16)
    whole = pltpu.VMEM((2, devices, 2, half, dim), BF16)
    table = pltpu.VMEM((2, devices, 2, half, hd), F32)

    def dmas(*shape):
        return pltpu.SemaphoreType.DMA(shape)

    scratch = [
        whole, whole,
        pltpu.VMEM((4, 2, half, dim), BF16),
        ring, ring,
        pltpu.VMEM(x.shape, BF16),
        table, table,
        pltpu.VMEM((2, 1, past), F32),
        pltpu.VMEM((n_q + 1, dim, TILE), BF16),
        pltpu.VMEM(wo.shape[1:], BF16),
        pltpu.VMEM((SLOTS, max(dim, DOWN * wd.shape[1]), TILE), BF16),
        pltpu.VMEM((devices, 2, half, wg.shape[2]), BF16),
        pltpu.VMEM((wq.shape[2] // hd, devices, 2, half, hd), BF16),
        pltpu.VMEM((chunk, wq.shape[2]), BF16),
        keys, keys,
        pltpu.VMEM((QROWS, past + chunk), F32),
        pltpu.VMEM((QROWS, hd), F32),
        pltpu.SemaphoreType.DMA, dmas(n_q + 3), dmas(SLOTS, DOWN), dmas(2), dmas(2), dmas(2, 2), pltpu.SemaphoreType.REGULAR,
    ]
    chips = [dmas(2, 2, 3)] * 2
    cores = [dmas(2, 2, 4)] * 2
    sends = [dmas(2, 2, 2, 3)]
    scratch += cores + chips + sends + sends + chips + cores
    return pl.pallas_call(
        layers_kernel,
        out_shape=(jax.ShapeDtypeStruct(x.shape, BF16),) + (jax.ShapeDtypeStruct((2, seqs, chunk, hd), BF16),) * 2,
        in_specs=[ANY, SMEM, VMEM, VMEM] + [ANY] * 11,
        out_specs=(ANY,) * 3,
        scratch_shapes=scratch,
        compiler_params=pltpu.CompilerParams(collective_id=0, has_side_effects=True, vmem_limit_bytes=LAYERS_LIMIT),
        name='layers',
    )(x, start, freq, norms, kl, vl, kg, vg, wq, wk, wv, wo, wg, wu, wd)


def cache_kernel(start_ref, x, k_new, v_new, kl, vl, kg, vg, x_o, kl_o, vl_o, kg_o, vg_o, xbuf, buf, fresh, s_x, s_in, s_fr, s_out):
    chunk = k_new.shape[2]
    window = kl.shape[1]
    lead = fresh.shape[1] - chunk
    n_buf = buf.shape[0]
    jobs = []
    for b in range(kl.shape[0]):
        for l, pairs in enumerate((((kl, k_new, kl_o), (vl, v_new, vl_o)), ((kg, k_new, kg_o), (vg, v_new, vg_o)))):
            jobs += [(src, new, dst, l, b) for src, new, dst in pairs]

    def load(i):
        src, new, _, l, b = jobs[i]
        k = i % n_buf
        return (pltpu.make_async_copy(src.at[b], buf.at[k, pl.ds(0, src.shape[1])], s_in.at[k]),
                pltpu.make_async_copy(new.at[l, b], fresh.at[k, pl.ds(0, chunk)], s_fr.at[k]))

    def store(i):
        src, _, dst, _, b = jobs[i]
        k = i % n_buf
        return pltpu.make_async_copy(buf.at[k, pl.ds(0, src.shape[1])], dst.at[b], s_out.at[k])

    x_in = pltpu.make_async_copy(x, xbuf, s_x)
    x_out = pltpu.make_async_copy(xbuf, x_o, s_x)
    x_in.start()
    for i in range(n_buf):
        for c in load(i):
            c.start()
    x_in.wait()
    x_out.start()
    for i, (_, _, _, l, b) in enumerate(jobs):
        k = i % n_buf
        for c in load(i):
            c.wait()
        start = start_ref[b]
        r = start % lead
        at = pl.multiple_of(start - r, lead)
        rolled = pltpu.roll(fresh[k].astype(F32), r, 0)
        row = lax.broadcasted_iota(jnp.int32, rolled.shape, 0)
        old = buf[k, pl.ds(at, chunk + lead)].astype(F32)
        buf[k, pl.ds(at, chunk + lead)] = jnp.where((row >= r) & (row < r + chunk), rolled, old).astype(BF16)
        if l == 0:
            over = buf[k, pl.ds(window, chunk)].astype(F32)
            row = lax.broadcasted_iota(jnp.int32, over.shape, 0)
            head = buf[k, pl.ds(0, chunk)].astype(F32)
            buf[k, pl.ds(0, chunk)] = jnp.where(row < start + chunk - window, over, head).astype(BF16)
        store(i).start()
        if i >= 1 and i - 1 + n_buf < len(jobs):
            store(i - 1).wait()
            for c in load(i - 1 + n_buf):
                c.start()
    for i in range(max(0, len(jobs) - n_buf), len(jobs)):
        store(i).wait()
    x_out.wait()


def write_caches(start, x, k_new, v_new, kl, vl, kg, vg):
    hd = kl.shape[2]
    chunk = k_new.shape[2]
    lead = 16
    depth = max(kl.shape[1] + chunk, kg.shape[1]) + lead
    n_buf = 8
    dmas = pltpu.SemaphoreType.DMA((n_buf,))
    return pl.pallas_call(
        cache_kernel,
        out_shape=tuple(jax.ShapeDtypeStruct(c.shape, BF16) for c in (x, kl, vl, kg, vg)),
        in_specs=[SMEM] + [ANY] * 7,
        out_specs=(ANY,) * 5,
        scratch_shapes=[pltpu.VMEM(x.shape, BF16), pltpu.VMEM((n_buf, depth, hd), BF16), pltpu.VMEM((n_buf, chunk + lead, hd), BF16),
                        pltpu.SemaphoreType.DMA, dmas, dmas, dmas],
        compiler_params=pltpu.CompilerParams(vmem_limit_bytes=VMEM_LIMIT),
        name='write_caches',
    )(start, x, k_new, v_new, kl, vl, kg, vg)


def solution(mesh):
    act_spec = P('dp', 'tp', None)
    cache_spec = P('dp', None, 'tp', None)
    col_spec = P(None, None, 'tp')
    row_spec = P(None, 'tp', None)
    arg_specs = (act_spec, P('dp'), cache_spec, cache_spec, cache_spec, cache_spec, P(), col_spec, col_spec, col_spec, row_spec, col_spec, col_spec, row_spec)
    result_specs = (act_spec, cache_spec, cache_spec, cache_spec, cache_spec)

    def device_step(x, start, k_local, v_local, k_global, v_global, norms, w_q, w_k, w_v, w_o, w_gate, w_up, w_down):
        hd = k_local.shape[3]
        freq = ROPE_BASE ** (np.arange(hd // 2) * (-2.0 / hd))
        freq = jnp.asarray(np.concatenate([freq, freq])[None], F32)
        flat = [c.reshape(c.shape[0], c.shape[1], hd) for c in (k_local, v_local, k_global, v_global)]
        x4 = x.reshape(x.shape[0], 2, x.shape[1] // 2, x.shape[2])
        x_out, k_new, v_new = run_layers(x4, start, freq, norms, *flat, w_q, w_k, w_v, w_o, w_gate, w_up, w_down)
        x_out = x_out.reshape(x.shape)
        x_out, *caches = write_caches(start, x_out, k_new, v_new, *flat)
        return (x_out,) + tuple(c.reshape(c.shape[0], c.shape[1], 1, hd) for c in caches)

    return jax.shard_map(device_step, mesh=mesh, in_specs=arg_specs, out_specs=result_specs, check_vma=False)
```

```python
import jax
import jax.numpy as jnp
import numpy as np
from jax import lax
from jax.experimental import pallas as pl
from jax.experimental.pallas import tpu as pltpu
from jax.sharding import PartitionSpec as P

SOFT_CAP = 50.0
NORM_EPS = 1e-6
ROPE_BASE = 10000.0
MASKED = -1e30
DIST = 2
LOWEST = -3e38
LOG2E = 1.4426950408889634

BF16 = jnp.bfloat16
F32 = jnp.float32
MESH_ID = pl.DeviceIdType.MESH
ANY = pl.BlockSpec(memory_space=pl.ANY)
VMEM = pl.BlockSpec(memory_space=pltpu.VMEM)
SMEM = pl.BlockSpec(memory_space=pltpu.SMEM)

TILE = 256
SLOTS = 5
DOWN = 2
SCORE_KEYS = 256
KEYS = 512
OUT = 2048
VMEM_LIMIT = 67_000_000
LAYERS_LIMIT = 67_000_000
SWAP = 1024
ATT_PLAN = ((2, 4), (10, 11), (7, 9), (14, 17), (14, 19), (18, 21), (19, 23), (21, 24), (24, 26))
MLP_PLAN = ((1, 2), (6, 6), (4, 5), (8, 8), (9, 10), (11, 11), (13, 13), (15, 15), (16, 16))
LEAVE = 4
GROUP = 2
HOLD_NS = 1000
SWAP_ORDER = (2, 1, 3, 0)
DO_COMPUTE = True
DO_COMM = True

PAIR = range(2)
LATER = (1, 2)


def mirror(table):
    return tuple(((4 - r) % 4, 1 - hh) for r, hh in table)


RS_RIGHT = ((2, 0), (1, 1), (1, 0))
RS_LEFT = mirror(RS_RIGHT)
AG_RIGHT = ((0, 0), (0, 1), (3, 0))
AG_LEFT = mirror(AG_RIGHT)
AG_FROM_LEFT = ((3, 0), (3, 1), (2, 0))
AG_FROM_RIGHT = mirror(AG_FROM_LEFT)


def repeat(n, body, low=0):
    lax.fori_loop(low, n, body, 0)


def dot(a, b):
    return jnp.dot(a, b, preferred_element_type=F32)


def dot_nt(a, b):
    return lax.dot_general(a, b, (((1,), (1,)), ((), ())), preferred_element_type=F32)


def layers_kernel(x_hbm, start_ref, freq_ref, norms_ref, kl_hbm, vl_hbm, kg_hbm, vg_hbm,
                  wq_hbm, wk_hbm, wv_hbm, wo_hbm, wg_hbm, wu_hbm, wd_hbm,
                  xo_hbm, kn_hbm, vn_hbm,
                  g, y, rb, ring_l, ring_r, xs, cos_ref, sin_ref, bias, wqkv, wo, slots, h_sc, q_sc, o_sc, kbuf, vbuf, t_sc, mx_sc,
                  s_x, s_attw, s_slot, s_kv, s_kvo, s_xo, credit,
                  rs_ds, rs_dr, rs_rl, rs_rr, rs_sr, ag_sr, ag_rl, ag_rr, ag_ds, ag_dr):
    _, devices, _, half, dim = g.shape
    chunk = devices * 2 * half
    piece = half // 2
    keys, hd = kbuf.shape
    past = keys - chunk
    n_q = wq_hbm.shape[2] // TILE
    heads = wq_hbm.shape[2] // hd
    ffn = wg_hbm.shape[2]
    n_up = ffn // TILE
    n_down = dim // TILE
    n_pairs = n_down // DOWN
    per_phase = 2 * n_up + n_pairs
    n_tiles = 4 * per_phase + n_pairs
    out_step = min(OUT, dim)
    swap_step = min(SWAP, dim)
    c1 = (hd ** -0.5) / SOFT_CAP
    c2 = SOFT_CAP * LOG2E

    dp = lax.axis_index('dp')
    me = lax.axis_index('tp')
    chip = me // 2
    core = me % 2
    chips = devices // 2
    right = (dp, (chip + 1) % chips * 2 + core)
    left = (dp, (chip + chips - 1) % chips * 2 + core)
    sibling = (dp, chip * 2 + 1 - core)
    partners = (sibling, left, right)

    def owner(offset, c):
        return (chip + offset) % chips * 2 + c

    def columns(first, size):
        return pl.ds(pl.multiple_of(first, TILE), size)

    def rows(hh):
        return pl.ds(pl.multiple_of(hh * piece, piece), piece)

    def push(src, dst, ssem, rsem, dev):
        return pltpu.make_async_remote_copy(src_ref=src, dst_ref=dst, send_sem=ssem, recv_sem=rsem, device_id=dev, device_id_type=MESH_ID)

    def att_weight_copies(l):
        out = [pltpu.make_async_copy(wq_hbm.at[l, :, pl.ds(i * TILE, TILE)], wqkv.at[i], s_attw.at[i]) for i in range(n_q)]
        out.append(pltpu.make_async_copy(wk_hbm.at[l], wqkv.at[n_q, :, pl.ds(0, hd)], s_attw.at[n_q]))
        out.append(pltpu.make_async_copy(wv_hbm.at[l], wqkv.at[n_q, :, pl.ds(hd, hd)], s_attw.at[n_q + 1]))
        out.append(pltpu.make_async_copy(wo_hbm.at[l], wo, s_attw.at[n_q + 2]))
        return out

    def cache_copies(k_hbm, v_hbm, s):
        return [pltpu.make_async_copy(c.at[s, pl.ds(0, past)], buf.at[pl.ds(0, past)], s_kv.at[i])
                for i, (c, buf) in enumerate(((k_hbm, kbuf), (v_hbm, vbuf)))]

    def start_tile(m):
        slot = m % SLOTS
        m = jnp.where(m < n_tiles - n_pairs, m, m - n_pairs)
        layer = m // (2 * per_phase)
        j = m % per_phase

        @pl.when((j < 2 * n_up) & (j % 2 == 0))
        def _():
            pltpu.make_async_copy(wg_hbm.at[layer, :, columns(j // 2 * TILE, TILE)], slots.at[slot, pl.ds(0, dim)], s_slot.at[slot, 0]).start()

        @pl.when((j < 2 * n_up) & (j % 2 == 1))
        def _():
            pltpu.make_async_copy(wu_hbm.at[layer, :, columns(j // 2 * TILE, TILE)], slots.at[slot, pl.ds(0, dim)], s_slot.at[slot, 0]).start()

        @pl.when(j >= 2 * n_up)
        def _():
            for i in range(DOWN):
                pltpu.make_async_copy(wd_hbm.at[layer, :, columns(((j - 2 * n_up) * DOWN + i) * TILE, TILE)],
                                      slots.at[slot, pl.ds(i * ffn, ffn)], s_slot.at[slot, i]).start()

    def next_tile(m):
        @pl.when(m + SLOTS < n_tiles)
        def _():
            start_tile(m + SLOTS)

    def wait_up_tile(slot):
        pltpu.make_async_copy(wg_hbm.at[0, :, pl.ds(0, TILE)], slots.at[slot, pl.ds(0, dim)], s_slot.at[slot, 0]).wait()

    def wait_down_pair(slot):
        for i in range(DOWN):
            pltpu.make_async_copy(wd_hbm.at[0, :, pl.ds(0, TILE)], slots.at[slot, pl.ds(i * ffn, ffn)], s_slot.at[slot, i]).wait()

    def swap(s, u, r, cols):
        return push(y.at[s, owner(r, 1 - core), u, :, cols], rb.at[r, u, :, cols], rs_ds.at[s, u, r], rs_dr.at[s, u, r], sibling)

    def swap_columns(s, u, first, size):
        if DO_COMM:
            for r in SWAP_ORDER:
                swap(s, u, r, columns(first, size)).start()

    def swapped(s, u, r):
        return swap(s, u, r, pl.ds(0, dim))

    def rs_right(s, u, k):
        r, hh = RS_RIGHT[k]
        return push(y.at[s, owner(r, core), u, rows(hh)], ring_l.at[u, k], rs_sr.at[s, u, 0, k], rs_rl.at[s, u, k], right)

    def rs_left(s, u, k):
        r, hh = RS_LEFT[k]
        return push(y.at[s, owner(r, core), u, rows(hh)], ring_r.at[u, k], rs_sr.at[s, u, 1, k], rs_rr.at[s, u, k], left)

    def add_in(dst, src):
        step = min(1024, dim)

        def body(i, carry):
            cols = pl.ds(pl.multiple_of(i * step, step), step)
            dst[:, cols] = (dst[:, cols].astype(F32) + src[:, cols].astype(F32)).astype(BF16)
            return carry

        repeat(dim // step, body)

    def fold(s, u, r):
        swapped(s, u, r).wait_recv()
        add_in(y.at[s, owner(r, core), u], rb.at[r, u])

    def rs1(s, u):
        fold(s, u, 2)
        rs_right(s, u, 0).start()
        rs_left(s, u, 0).start()

    def rs2(s, u):
        fold(s, u, 1)
        rs_right(s, u, 1).start()
        fold(s, u, 3)
        rs_left(s, u, 1).start()

    def rs3(s, u):
        rs_right(s, u, 0).wait_recv()
        add_in(y.at[s, owner(1, core), u, rows(0)], ring_l.at[u, 0])
        rs_right(s, u, 2).start()
        rs_left(s, u, 0).wait_recv()
        add_in(y.at[s, owner(3, core), u, rows(1)], ring_r.at[u, 0])
        rs_left(s, u, 2).start()

    def rs4_wait(s, u):
        swapped(s, u, 0).wait_recv()
        for k in LATER:
            rs_right(s, u, k).wait_recv()
            rs_left(s, u, k).wait_recv()

    def rs_drain(s):
        for u in PAIR:
            for r in range(4):
                swapped(s, u, r).wait_send()
            for k in range(3):
                rs_right(s, u, k).wait_send()
                rs_left(s, u, k).wait_send()

    def norm_row(i):
        return norms_ref[i // 4, pl.ds(i % 4, 1)]

    def inv_rms(v):
        return lax.rsqrt(jnp.sum(v * v, axis=-1, keepdims=True) * (1.0 / dim) + NORM_EPS)

    def finish(s, u, post, has_next):
        def body(hh, carry):
            at = rows(hh)
            total = (y[s, me, u, at].astype(F32) + rb[0, u, at].astype(F32)
                     + ring_l[u, 2 - hh].astype(F32) + ring_r[u, 1 + hh].astype(F32))
            v = total.astype(BF16).astype(F32)
            x1 = (xs[s, u, at].astype(F32) + v * inv_rms(v) * (1.0 + norm_row(post))).astype(BF16)
            xs[s, u, at] = x1
            if has_next:
                w = x1.astype(F32)
                g[s, me, u, at] = (w * inv_rms(w) * (1.0 + norm_row(post + 1))).astype(BF16)
            return carry

        repeat(2, body)

    def ag_right(t, u, k, table=AG_RIGHT):
        r, hh = table[k]
        ref = g.at[t, owner(r, core), u, rows(hh)]
        return push(ref, ref, ag_sr.at[t, u, 0, k], ag_rl.at[t, u, k], right)

    def ag_left(t, u, k, table=AG_LEFT):
        r, hh = table[k]
        ref = g.at[t, owner(r, core), u, rows(hh)]
        return push(ref, ref, ag_sr.at[t, u, 1, k], ag_rr.at[t, u, k], left)

    def from_left(t, u, k):
        ag_right(t, u, k, AG_FROM_LEFT).wait_recv()

    def from_right(t, u, k):
        ag_left(t, u, k, AG_FROM_RIGHT).wait_recv()

    def ag_d2d(t, u, r, c):
        ref = g.at[t, owner(r, c), u]
        return push(ref, ref, ag_ds.at[t, u, r], ag_dr.at[t, u, r], sibling)

    def ag_out(t, u, k):
        ag_right(t, u, k).start()
        ag_left(t, u, k).start()

    def ag_gone(t, u, k):
        ag_right(t, u, k).wait_send()
        ag_left(t, u, k).wait_send()

    def ag1(t, u):
        for k in PAIR:
            ag_out(t, u, k)
        ag_d2d(t, u, 0, core).start()

    def ag2(t, u):
        from_left(t, u, 0)
        ag_right(t, u, 2).start()
        from_right(t, u, 0)
        ag_left(t, u, 2).start()

    def ag3(t, u):
        from_left(t, u, 1)
        ag_d2d(t, u, 3, core).start()
        from_right(t, u, 1)
        ag_d2d(t, u, 1, core).start()

    def ag4(t, u):
        from_left(t, u, 2)
        from_right(t, u, 2)
        ag_d2d(t, u, 2, core).start()

    def ag_own(t):
        for u in PAIR:
            ag_d2d(t, u, 0, 1 - core).wait_recv()

    def ag5(t, u):
        for r in (1, 3, 2):
            ag_d2d(t, u, r, 1 - core).wait_recv()

    def ag_drain(t, first):
        for u in PAIR:
            pl.when(jnp.logical_not(first))(lambda: ag_gone(t, u, 0))
            for k in LATER:
                ag_gone(t, u, k)
            for r in range(4):
                ag_d2d(t, u, r, core).wait_send()

    def rows_of(v):
        return v.reshape(chunk // 2, v.shape[-1])

    def rope(v, s, u):
        return v * rows_of(cos_ref[s, :, u]) + pltpu.roll(v, hd // 2, 1) * rows_of(sin_ref[s, :, u])

    def project_q(i, u, s):
        p = dot(rows_of(g[s, :, u]), wqkv[i])
        for hh in range(TILE // hd):
            rot = rope(p[:, hh * hd:(hh + 1) * hd], s, u).astype(BF16)
            q_sc[i * (TILE // hd) + hh, :, u] = rot.reshape(devices, half, hd)

    def project_kv(u, s):
        p = dot(rows_of(g[s, :, u]), wqkv[n_q])
        k = rope(p[:, :hd], s, u).astype(BF16).reshape(devices, half, hd)
        v = p[:, hd:].astype(BF16).reshape(devices, half, hd)
        for j in range(devices):
            at = pl.ds(past + (2 * j + u) * half, half)
            kbuf[at] = k[j]
            vbuf[at] = v[j]

    def fresh_out(s, l):
        return [pltpu.make_async_copy(buf.at[pl.ds(past, chunk)], out.at[l, s], s_kvo.at[i])
                for i, (buf, out) in enumerate(((kbuf, kn_hbm), (vbuf, vn_hbm)))]

    def scores(head, u, s, l):
        row = lax.broadcasted_iota(jnp.int32, (chunk // 2, SCORE_KEYS), 0)
        token = row + jnp.bitwise_and(row, -half) + u * half
        diff = lax.broadcasted_iota(jnp.int32, (chunk // 2, SCORE_KEYS), 1) - token
        oldest = jnp.where(l == 0, start_ref[s] - past, -past)
        q = rows_of(q_sc[head, :, u])
        top = None
        for kb in range((past + chunk) // SCORE_KEYS):
            first = kb * SCORE_KEYS
            cols = pl.ds(first, SCORE_KEYS)
            t = jnp.tanh(dot_nt(q, kbuf[cols]) * c1) * c2
            if past // 2 <= first < past:
                t = t + bias[s, :, cols]
            if first < chunk:
                t = jnp.where(diff > oldest - first, t, MASKED)
            if first >= past:
                t = jnp.where(diff <= past - first, t, MASKED)
            t_sc[:, cols] = t
            for i in range(SCORE_KEYS // hd):
                ti = t[:, i * hd:(i + 1) * hd]
                top = ti if top is None else jnp.maximum(top, ti)
        mx_sc[...] = top

    def weigh(head, u):
        mc = jnp.max(mx_sc[...], axis=-1, keepdims=True)
        mc = jnp.broadcast_to(mc, (chunk // 2, hd))
        n_kb = (past + chunk) // KEYS
        total = acc = None
        pvs = []
        for kb in range(n_kb):
            cols = pl.ds(kb * KEYS, KEYS)
            if kb >= DIST:
                mc = jnp.maximum(mc, jnp.minimum(pvs[kb - DIST], LOWEST))
            ps = []
            for i in range(KEYS // hd):
                pi = jnp.exp2(t_sc[:, pl.ds(kb * KEYS + i * hd, hd)] - mc)
                total = pi if total is None else total + pi
                ps.append(pi.astype(BF16))
            pv = dot(jnp.concatenate(ps, axis=1), vbuf[cols])
            pvs.append(pv)
            acc = pv if acc is None else acc + pv
        o = acc / jnp.sum(total, axis=-1, keepdims=True)
        o_sc[:, u, :, pl.ds(pl.multiple_of(head * hd, hd), hd)] = o.astype(BF16).reshape(devices, half, hd)

    def out_tile(i, u, s):
        cols = columns(i * out_step, out_step)
        y[s, :, u, :, cols] = dot(rows_of(o_sc[:, u]), wo[:, cols]).astype(BF16).reshape(devices, half, out_step)

    def gated(x, sa, sb):
        return (jax.nn.gelu(dot(x, slots[sa, pl.ds(0, dim)]), approximate=True) * dot(x, slots[sb, pl.ds(0, dim)])).astype(BF16)

    def up_half(jj, u, s, m0):
        m = m0 + 2 * jj
        h_sc[:, u, :, columns(jj * TILE, TILE)] = gated(rows_of(g[s, :, u]), m % SLOTS, (m + 1) % SLOTS).reshape(devices, half, TILE)

    def up_tile(jj, s, m0):
        m = m0 + 2 * jj
        wait_up_tile(m % SLOTS)
        wait_up_tile((m + 1) % SLOTS)
        h = gated(g[s].reshape(chunk, dim), m % SLOTS, (m + 1) % SLOTS)
        h_sc[:, :, :, columns(jj * TILE, TILE)] = h.reshape(devices, 2, half, TILE)
        next_tile(m)
        next_tile(m + 1)

    def down_pairs(n, count, s, m0, u=None):
        m = m0 + 2 * n_up + n
        for i in range(count):
            wait_down_pair((m + i) % SLOTS)
        for i in range(count * DOWN):
            cols = columns((n % n_pairs * DOWN + i) * TILE, TILE)
            w = slots[(m + i // DOWN) % SLOTS, pl.ds(i % DOWN * ffn, ffn)]
            if u is None:
                y[s, :, :, :, cols] = dot(h_sc[...].reshape(chunk, ffn), w).astype(BF16).reshape(devices, 2, half, TILE)
            else:
                y[s, :, u, :, cols] = dot(rows_of(h_sc[:, u]), w).astype(BF16).reshape(devices, half, TILE)
        for i in range(count):
            next_tile(m + i)

    def settle(t, u, post, gather):
        rs4_wait(t, u)

        @pl.when(gather)
        def _():
            finish(t, u, post, True)
            ag1(t, u)

        @pl.when(jnp.logical_not(gather))
        def _():
            finish(t, u, post, False)

    def events(t, post, reduce, early, gather):
        def onward():
            rs3(t, 0)
            pl.when(jnp.logical_not(early))(lambda: rs2(t, 1))

        def if_reduce(what):
            return lambda: pl.when(reduce)(what)

        def if_gather(f, u):
            return lambda: pl.when(gather)(lambda: f(t, u))

        return (if_reduce(onward), if_reduce(lambda: settle(t, 0, post, gather)), if_reduce(lambda: rs3(t, 1)),
                if_reduce(lambda: settle(t, 1, post, gather)),
                if_gather(ag2, 0), if_gather(ag3, 0), if_gather(ag2, 1), if_gather(ag3, 1), if_gather(ag4, 0))

    def at(step, low, high, early, plan, todo):
        if DO_COMM:
            for (soon, late), what in sorted(zip(plan, todo), key=lambda e: e[0][1]):
                if low <= soon < high or low <= late < high:
                    pl.when(step == jnp.where(early, soon, late))(what)

    def rest(early, plan, todo, last):
        for (soon, late), what in zip(plan, todo):
            if max(soon, late) >= last:
                pl.when(jnp.where(early, soon, late) >= last)(what)

    def att_phase(l, s):
        t = 1 - s
        reduce = (l > 0) | (s > 0)
        early = l == 0
        todo = events(t, 4 * l - 1 + 2 * s, reduce, early, l >= 0)
        n_proj = n_q + 1
        n_out = dim // out_step
        first_block = 2 * n_proj
        per_half = 2 * heads + n_out
        last = first_block + 2 * per_half
        if DO_COMPUTE:
            for c in att_weight_copies(l)[:-1]:
                pl.when(s == 0)(c.wait)
        if DO_COMM:
            ag5(s, 0)

        def proj(i, carry):
            if DO_COMPUTE:
                pl.when(i % n_proj < n_q)(lambda: project_q(i % n_proj, i // n_proj, s))
                pl.when(i % n_proj == n_q)(lambda: project_kv(i // n_proj, s))
            if DO_COMM:
                pl.when(i == 0)(lambda: ag4(s, 1))

                @pl.when(i == n_proj - 1)
                def _():
                    ag5(s, 1)
                    ag_drain(s, (l == 0) & (s == 0))
            at(i, 0, first_block, early, ATT_PLAN, todo)
            return carry

        repeat(first_block, proj)
        if DO_COMPUTE:
            for c in fresh_out(s, l):
                c.start()
            for c in cache_copies(kl_hbm, vl_hbm, s):
                c.wait()
        for u in PAIR:
            low = first_block + u * per_half

            def blk(i, carry):
                if DO_COMPUTE:
                    pl.when(i % 2 == 0)(lambda: scores(i // 2, u, s, l))
                    pl.when(i % 2 == 1)(lambda: weigh(i // 2, u))
                at(low + i, low, low + 2 * heads, early, ATT_PLAN, todo)
                if DO_COMM and u == 1:
                    @pl.when(early & (i == 1))
                    def _():
                        ag_own(t)
                        swap_columns(s, 0, 0, dim)

                    @pl.when(early & (i == LEAVE))
                    def _():
                        rs1(s, 0)
                        rs2(s, 0)
                return carry

            repeat(2 * heads, blk)
            if DO_COMPUTE and u == 0:
                pl.when(s == 0)(att_weight_copies(l)[-1].wait)
            if DO_COMPUTE and u == 1:
                for c in fresh_out(s, l):
                    c.wait()

                @pl.when((l == 0) & (s == 0))
                def _():
                    for c in cache_copies(kl_hbm, vl_hbm, 1):
                        c.start()

                @pl.when(l + s == 1)
                def _():
                    for c in cache_copies(kg_hbm, vg_hbm, l):
                        c.start()
            if DO_COMM:
                if u == 1:
                    pl.when(jnp.logical_not(early))(lambda: ag_own(t))

            def out_body(i, carry):
                if DO_COMPUTE:
                    out_tile(i, u, s)
                for j in range(out_step // swap_step):
                    first = i * out_step + j * swap_step
                    if u == 1:
                        pl.when(jnp.logical_not(early))(lambda: swap_columns(s, 0, first, swap_step))
                        swap_columns(s, 1, first, swap_step)
                at(low + 2 * heads + i, low + 2 * heads, low + per_half, early, ATT_PLAN, todo)
                return carry

            repeat(n_out, out_body)
        if DO_COMPUTE:
            @pl.when((s == 1) & (l == 0))
            def _():
                for c in att_weight_copies(1):
                    c.start()
        if DO_COMM:
            @pl.when(early)
            def _():
                rs1(s, 1)
                rs2(s, 1)

            @pl.when(jnp.logical_not(early))
            def _():
                rs1(s, 0)
                rs2(s, 0)
                rs1(s, 1)
            rest(early, ATT_PLAN, todo, last)
            pl.when(reduce)(lambda: rs_drain(t))

    def mlp_phase(l, s):
        t = 1 - s
        m0 = (2 * l + s) * per_phase
        gather = (l == 0) | (s == 0)
        early = l + s == 0
        todo = events(t, 4 * l + 1 + 2 * s, l >= 0, early, gather)
        first_down = n_up + 2
        last = first_down + n_pairs
        if DO_COMM:
            ag5(s, 0)

        def halves(i, carry):
            if DO_COMPUTE:
                m = m0 + 2 * i

                @pl.when(i < 2)
                def _():
                    wait_up_tile(m % SLOTS)
                    wait_up_tile((m + 1) % SLOTS)
                up_half(i % 2, i // 2, s, m0)

                @pl.when(i >= 2)
                def _():
                    next_tile(m - 4)
                    next_tile(m - 3)
            if DO_COMM:
                pl.when(i == 0)(lambda: ag4(s, 1))

                @pl.when(i == 1)
                def _():
                    ag5(s, 1)
                    ag_drain(s, l < 0)
            at(i, 0, 4, early, MLP_PLAN, todo)
            return carry

        repeat(4, halves)

        def ups(jj, carry):
            if DO_COMPUTE:
                up_tile(jj, s, m0)
            at(2 + jj, 4, first_down, early, MLP_PLAN, todo)
            return carry

        repeat(n_up, ups, 2)

        every = swap_step // (DOWN * TILE)

        @pl.when(gather)
        def _():
            def downs(n, carry):
                if DO_COMPUTE:
                    down_pairs(n, 1, s, m0)
                if DO_COMM:
                    pl.when(n == every - 1)(lambda: ag_own(t))

                @pl.when(n % every == every - 1)
                def _():
                    for u in PAIR:
                        swap_columns(s, u, n // every * swap_step, swap_step)
                at(first_down + n, first_down, last, early, MLP_PLAN, todo)
                return carry

            repeat(n_pairs, downs)
            if DO_COMM:
                rs1(s, 0)
                rs2(s, 0)
                rs1(s, 1)
                rest(early, MLP_PLAN, todo, last)

        @pl.when(jnp.logical_not(gather))
        def _():
            if DO_COMM:
                rest(early, MLP_PLAN[:4], todo, first_down)
                for dev in partners:
                    pl.semaphore_signal(credit, inc=1, device_id=dev, device_id_type=MESH_ID)
            n_steps = n_pairs // GROUP
            rare = max(n_steps // 2, 1)
            width = rare * GROUP * DOWN * TILE
            for u in PAIR:
                def downs(n, carry):
                    if DO_COMPUTE:
                        down_pairs(u * n_pairs + n * GROUP, GROUP, s, m0, u)
                    if DO_COMM:
                        if u == 0:
                            pl.when(n == rare - 1)(lambda: pl.semaphore_wait(credit, len(partners)))
                        pl.when(n % rare == rare - 1)(lambda: swap_columns(s, u, n // rare * width, width))
                        if u == 1:
                            @pl.when(n == 0)
                            def _():
                                rs1(s, 0)
                                rs2(s, 0)
                    return carry

                repeat(n_steps, downs)
            if DO_COMM:
                rs1(s, 1)
                rs3(s, 0)
                fold(s, 1, 1)
                fold(s, 1, 3)
                pl.delay(HOLD_NS)
                rs_right(s, 1, 1).start()
                rs_left(s, 1, 1).start()
        if DO_COMM:
            rs_drain(t)

    xcopy = pltpu.make_async_copy(x_hbm, xs, s_x)
    xcopy.start()
    barrier = pltpu.get_barrier_semaphore()
    for dev in partners:
        pl.semaphore_signal(barrier, inc=1, device_id=dev, device_id_type=MESH_ID)

    def first_norm(s, u):
        def body(hh, carry):
            v = xs[s, u, rows(hh)].astype(F32)
            g[s, me, u, rows(hh)] = (v * inv_rms(v) * (1.0 + norm_row(0))).astype(BF16)
            return carry

        repeat(2, body)

    xcopy.wait()
    first_norm(0, 0)
    pl.semaphore_wait(barrier, len(partners))
    for u in PAIR:
        if u == 1:
            first_norm(0, 1)
        if DO_COMM:
            ag_out(0, u, 0)
            ag_d2d(0, u, 0, core).start()
    if DO_COMPUTE:
        for c in att_weight_copies(0) + cache_copies(kl_hbm, vl_hbm, 0):
            c.start()
        for m in range(SLOTS):
            start_tile(jnp.int32(m))
    for u in PAIR:
        first_norm(1, u)
    for s in PAIR:
        shape = cos_ref.shape[1:]
        pos = start_ref[s] + sum(n * lax.broadcasted_iota(jnp.int32, shape, i) for i, n in enumerate((2 * half, half, 1)))
        angle = pos.astype(F32) * freq_ref[...]
        cos_ref[s] = jnp.cos(angle)
        sin = jnp.sin(angle)
        sin_ref[s] = jnp.where(lax.broadcasted_iota(jnp.int32, shape, 3) < hd // 2, -sin, sin)
        bias[s] = jnp.where(lax.broadcasted_iota(jnp.int32, (1, past), 1) < start_ref[s], 0.0, MASKED)
    if DO_COMM:
        for u in PAIR:
            ag_gone(0, u, 0)
            ag_out(0, u, 1)
        for u in PAIR:
            ag2(0, u)
        for u in PAIR:
            ag3(0, u)
        ag4(0, 0)
        ag_own(0)
        for u in PAIR:
            ag1(1, u)

    def layer(l, carry):
        def att(s, carry):
            att_phase(l, s)
            return carry

        def mlp(s, carry):
            mlp_phase(l, s)
            return carry

        repeat(2, att)
        repeat(2, mlp)
        return carry

    repeat(2, layer)

    out = [pltpu.make_async_copy(xs.at[s, u], xo_hbm.at[s, u], s_xo.at[s, u]) for s in PAIR for u in PAIR]
    out[0].start()
    out[1].start()
    for u in PAIR:
        if DO_COMM:
            if u == 1:
                rs3(1, 1)
            rs4_wait(1, u)
            finish(1, u, 7, False)
        out[2 + u].start()
    if DO_COMM:
        rs_drain(1)
    for copy in out:
        copy.wait()


def run_layers(x, start, freq, norms, kl, vl, kg, vg, wq, wk, wv, wo, wg, wu, wd):
    seqs, _, half, dim = x.shape
    _, past, hd = kl.shape
    chunk = kg.shape[1] - past
    n_q = wq.shape[2] // TILE
    devices = chunk // (2 * half)
    ring = pltpu.VMEM((2, 3, half // 2, dim), BF16)
    keys = pltpu.VMEM((past + chunk, hd), BF16)
    whole = pltpu.VMEM((2, devices, 2, half, dim), BF16)
    table = pltpu.VMEM((2, devices, 2, half, hd), F32)

    def dmas(*shape):
        return pltpu.SemaphoreType.DMA(shape)

    scratch = [
        whole, whole,
        pltpu.VMEM((4, 2, half, dim), BF16),
        ring, ring,
        pltpu.VMEM(x.shape, BF16),
        table, table,
        pltpu.VMEM((2, 1, past), F32),
        pltpu.VMEM((n_q + 1, dim, TILE), BF16),
        pltpu.VMEM(wo.shape[1:], BF16),
        pltpu.VMEM((SLOTS, max(dim, DOWN * wd.shape[1]), TILE), BF16),
        pltpu.VMEM((devices, 2, half, wg.shape[2]), BF16),
        pltpu.VMEM((wq.shape[2] // hd, devices, 2, half, hd), BF16),
        pltpu.VMEM((devices, 2, half, wq.shape[2]), BF16),
        keys, keys,
        pltpu.VMEM((chunk // 2, past + chunk), F32),
        pltpu.VMEM((chunk // 2, hd), F32),
        pltpu.SemaphoreType.DMA, dmas(n_q + 3), dmas(SLOTS, DOWN), dmas(2), dmas(2), dmas(2, 2), pltpu.SemaphoreType.REGULAR,
    ]
    chips = [dmas(2, 2, 3)] * 2
    cores = [dmas(2, 2, 4)] * 2
    sends = [dmas(2, 2, 2, 3)]
    scratch += cores + chips + sends + sends + chips + cores
    return pl.pallas_call(
        layers_kernel,
        out_shape=(jax.ShapeDtypeStruct(x.shape, BF16),) + (jax.ShapeDtypeStruct((2, seqs, chunk, hd), BF16),) * 2,
        in_specs=[ANY, SMEM, VMEM, VMEM] + [ANY] * 11,
        out_specs=(ANY,) * 3,
        scratch_shapes=scratch,
        compiler_params=pltpu.CompilerParams(collective_id=0, has_side_effects=True, vmem_limit_bytes=LAYERS_LIMIT),
        name='layers',
    )(x, start, freq, norms, kl, vl, kg, vg, wq, wk, wv, wo, wg, wu, wd)


def cache_kernel(start_ref, x, k_new, v_new, kl, vl, kg, vg, x_o, kl_o, vl_o, kg_o, vg_o, xbuf, buf, fresh, s_x, s_in, s_fr, s_out):
    _, _, chunk, _ = k_new.shape
    _, window, _ = kl.shape
    lead = fresh.shape[1] - chunk
    n_buf = buf.shape[0]
    jobs = []
    for b in range(kl.shape[0]):
        for l, pairs in enumerate((((kl, k_new, kl_o), (vl, v_new, vl_o)), ((kg, k_new, kg_o), (vg, v_new, vg_o)))):
            jobs += [(src, new, dst, l, b) for src, new, dst in pairs]

    def load(i):
        src, new, _, l, b = jobs[i]
        k = i % n_buf
        return (pltpu.make_async_copy(src.at[b], buf.at[k, pl.ds(0, src.shape[1])], s_in.at[k]),
                pltpu.make_async_copy(new.at[l, b], fresh.at[k, pl.ds(0, chunk)], s_fr.at[k]))

    def store(i):
        src, _, dst, _, b = jobs[i]
        k = i % n_buf
        return pltpu.make_async_copy(buf.at[k, pl.ds(0, src.shape[1])], dst.at[b], s_out.at[k])

    x_in = pltpu.make_async_copy(x, xbuf, s_x)
    x_out = pltpu.make_async_copy(xbuf, x_o, s_x)
    x_in.start()
    for i in range(n_buf):
        for c in load(i):
            c.start()
    x_in.wait()
    x_out.start()
    for i, (_, _, _, l, b) in enumerate(jobs):
        k = i % n_buf
        for c in load(i):
            c.wait()
        start = start_ref[b]
        r = start % lead
        at = pl.multiple_of(start - r, lead)
        rolled = pltpu.roll(fresh[k].astype(F32), r, 0)
        row = lax.broadcasted_iota(jnp.int32, rolled.shape, 0)
        old = buf[k, pl.ds(at, chunk + lead)].astype(F32)
        buf[k, pl.ds(at, chunk + lead)] = jnp.where((row >= r) & (row < r + chunk), rolled, old).astype(BF16)
        if l == 0:
            over = buf[k, pl.ds(window, chunk)].astype(F32)
            row = lax.broadcasted_iota(jnp.int32, over.shape, 0)
            head = buf[k, pl.ds(0, chunk)].astype(F32)
            buf[k, pl.ds(0, chunk)] = jnp.where(row < start + chunk - window, over, head).astype(BF16)
        store(i).start()
        if i >= 1 and i - 1 + n_buf < len(jobs):
            store(i - 1).wait()
            for c in load(i - 1 + n_buf):
                c.start()
    for i in range(max(0, len(jobs) - n_buf), len(jobs)):
        store(i).wait()
    x_out.wait()


def write_caches(start, x, k_new, v_new, kl, vl, kg, vg):
    _, _, hd = kl.shape
    _, _, chunk, _ = k_new.shape
    lead = 16
    depth = max(kl.shape[1] + chunk, kg.shape[1]) + lead
    n_buf = 8
    dmas = pltpu.SemaphoreType.DMA((n_buf,))
    return pl.pallas_call(
        cache_kernel,
        out_shape=tuple(jax.ShapeDtypeStruct(c.shape, BF16) for c in (x, kl, vl, kg, vg)),
        in_specs=[SMEM] + [ANY] * 7,
        out_specs=(ANY,) * 5,
        scratch_shapes=[pltpu.VMEM(x.shape, BF16), pltpu.VMEM((n_buf, depth, hd), BF16), pltpu.VMEM((n_buf, chunk + lead, hd), BF16),
                        pltpu.SemaphoreType.DMA, dmas, dmas, dmas],
        compiler_params=pltpu.CompilerParams(vmem_limit_bytes=VMEM_LIMIT),
        name='write_caches',
    )(start, x, k_new, v_new, kl, vl, kg, vg)


def solution(mesh):
    act_spec = P('dp', 'tp', None)
    cache_spec = P('dp', None, 'tp', None)
    col_spec = P(None, None, 'tp')
    row_spec = P(None, 'tp', None)
    arg_specs = (act_spec, P('dp'), cache_spec, cache_spec, cache_spec, cache_spec, P(), col_spec, col_spec, col_spec, row_spec, col_spec, col_spec, row_spec)
    result_specs = (act_spec, cache_spec, cache_spec, cache_spec, cache_spec)

    def device_step(x, start, k_local, v_local, k_global, v_global, norms, w_q, w_k, w_v, w_o, w_gate, w_up, w_down):
        hd = k_local.shape[3]
        freq = ROPE_BASE ** (np.arange(hd // 2) * (-2.0 / hd))
        freq = jnp.asarray(np.concatenate([freq, freq])[None], F32)
        flat = [c.reshape(c.shape[0], c.shape[1], hd) for c in (k_local, v_local, k_global, v_global)]
        x4 = x.reshape(x.shape[0], 2, x.shape[1] // 2, x.shape[2])
        x_out, k_new, v_new = run_layers(x4, start, freq, norms, *flat, w_q, w_k, w_v, w_o, w_gate, w_up, w_down)
        x_out = x_out.reshape(x.shape)
        x_out, *caches = write_caches(start, x_out, k_new, v_new, *flat)
        return (x_out,) + tuple(c.reshape(c.shape[0], c.shape[1], 1, hd) for c in caches)

    return jax.shard_map(device_step, mesh=mesh, in_specs=arg_specs, out_specs=result_specs, check_vma=False)
```

```python
import jax
import jax.numpy as jnp
import numpy as np
from jax import lax
from jax.experimental import pallas as pl
from jax.experimental.pallas import tpu as pltpu
from jax.sharding import PartitionSpec as P

SOFT_CAP = 50.0
NORM_EPS = 1e-6
ROPE_BASE = 10000.0
MASKED = -1e30
DIST = 2
LOWEST = -3e38
LOG2E = 1.4426950408889634

BF16 = jnp.bfloat16
F32 = jnp.float32
MESH_ID = pl.DeviceIdType.MESH
ANY = pl.BlockSpec(memory_space=pl.ANY)
VMEM = pl.BlockSpec(memory_space=pltpu.VMEM)
SMEM = pl.BlockSpec(memory_space=pltpu.SMEM)

TILE = 256
SLOTS = 5
DOWN = 2
SCORE_KEYS = 256
KEYS = 512
OUT = 2048
VMEM_LIMIT = 67_000_000
LAYERS_LIMIT = 67_000_000
SWAP = 1024
ATT_PLAN = ((2, 4), (10, 11), (7, 9), (14, 17), (14, 19), (18, 21), (19, 23), (21, 24), (24, 26))
MLP_PLAN = ((1, 2), (6, 6), (4, 5), (8, 8), (9, 10), (11, 11), (13, 13), (15, 15), (16, 16))
LEAVE = 4
GROUP = 2
HOLD_NS = 1000
SWAP_ORDER = (2, 1, 3, 0)
DO_COMPUTE = True
DO_COMM = True

PAIR = range(2)
LATER = (1, 2)


def mirror(table):
    return tuple(((4 - r) % 4, 1 - hh) for r, hh in table)


RS_RIGHT = ((2, 0), (1, 1), (1, 0))
RS_LEFT = mirror(RS_RIGHT)
AG_RIGHT = ((0, 0), (0, 1), (3, 0))
AG_LEFT = mirror(AG_RIGHT)
AG_FROM_LEFT = ((3, 0), (3, 1), (2, 0))
AG_FROM_RIGHT = mirror(AG_FROM_LEFT)


def repeat(n, body, low=0):
    lax.fori_loop(low, n, body, 0)


def dot(a, b):
    return jnp.dot(a, b, preferred_element_type=F32)


def dot_nt(a, b):
    return lax.dot_general(a, b, (((1,), (1,)), ((), ())), preferred_element_type=F32)


def layers_kernel(x_hbm, start_ref, freq_hbm, norms_hbm, kl_hbm, vl_hbm, kg_hbm, vg_hbm,
                  wq_hbm, wk_hbm, wv_hbm, wo_hbm, wg_hbm, wu_hbm, wd_hbm,
                  xo_hbm, kn_hbm, vn_hbm,
                  g, y, rb, ring_l, ring_r, xs, norms_ref, freq_ref, cos_ref, sin_ref, bias, wqkv, wo, slots, h_sc, q_sc, o_sc, kbuf, vbuf, t_sc, mx_sc,
                  s_x, s_attw, s_slot, s_kv, s_kvo, s_xo, credit,
                  rs_ds, rs_dr, rs_rl, rs_rr, rs_sr, ag_sr, ag_rl, ag_rr, ag_ds, ag_dr):
    _, devices, _, half, dim = g.shape
    chunk = devices * 2 * half
    piece = half // 2
    keys, hd = kbuf.shape
    past = keys - chunk
    n_q = wq_hbm.shape[2] // TILE
    heads = wq_hbm.shape[2] // hd
    ffn = wg_hbm.shape[2]
    n_up = ffn // TILE
    n_down = dim // TILE
    n_pairs = n_down // DOWN
    per_phase = 2 * n_up + n_pairs
    n_tiles = 4 * per_phase + n_pairs
    out_step = min(OUT, dim)
    swap_step = min(SWAP, dim)
    c1 = (hd ** -0.5) / SOFT_CAP
    c2 = SOFT_CAP * LOG2E

    dp = lax.axis_index('dp')
    me = lax.axis_index('tp')
    chip = me // 2
    core = me % 2
    chips = devices // 2
    right = (dp, (chip + 1) % chips * 2 + core)
    left = (dp, (chip + chips - 1) % chips * 2 + core)
    sibling = (dp, chip * 2 + 1 - core)
    partners = (sibling, left, right)

    def owner(offset, c):
        return (chip + offset) % chips * 2 + c

    def columns(first, size):
        return pl.ds(pl.multiple_of(first, TILE), size)

    def rows(hh):
        return pl.ds(pl.multiple_of(hh * piece, piece), piece)

    def push(src, dst, ssem, rsem, dev):
        return pltpu.make_async_remote_copy(src_ref=src, dst_ref=dst, send_sem=ssem, recv_sem=rsem, device_id=dev, device_id_type=MESH_ID)

    def att_weight_copies(l):
        out = [pltpu.make_async_copy(wq_hbm.at[l, :, pl.ds(i * TILE, TILE)], wqkv.at[i], s_attw.at[i]) for i in range(n_q)]
        out.append(pltpu.make_async_copy(wk_hbm.at[l], wqkv.at[n_q, :, pl.ds(0, hd)], s_attw.at[n_q]))
        out.append(pltpu.make_async_copy(wv_hbm.at[l], wqkv.at[n_q, :, pl.ds(hd, hd)], s_attw.at[n_q + 1]))
        out.append(pltpu.make_async_copy(wo_hbm.at[l], wo, s_attw.at[n_q + 2]))
        return out

    def cache_copies(k_hbm, v_hbm, s):
        return [pltpu.make_async_copy(c.at[s, pl.ds(0, past)], buf.at[pl.ds(0, past)], s_kv.at[i])
                for i, (c, buf) in enumerate(((k_hbm, kbuf), (v_hbm, vbuf)))]

    def start_tile(m):
        slot = m % SLOTS
        m = jnp.where(m < n_tiles - n_pairs, m, m - n_pairs)
        layer = m // (2 * per_phase)
        j = m % per_phase

        @pl.when((j < 2 * n_up) & (j % 2 == 0))
        def _():
            pltpu.make_async_copy(wg_hbm.at[layer, :, columns(j // 2 * TILE, TILE)], slots.at[slot, pl.ds(0, dim)], s_slot.at[slot, 0]).start()

        @pl.when((j < 2 * n_up) & (j % 2 == 1))
        def _():
            pltpu.make_async_copy(wu_hbm.at[layer, :, columns(j // 2 * TILE, TILE)], slots.at[slot, pl.ds(0, dim)], s_slot.at[slot, 0]).start()

        @pl.when(j >= 2 * n_up)
        def _():
            for i in range(DOWN):
                pltpu.make_async_copy(wd_hbm.at[layer, :, columns(((j - 2 * n_up) * DOWN + i) * TILE, TILE)],
                                      slots.at[slot, pl.ds(i * ffn, ffn)], s_slot.at[slot, i]).start()

    def next_tile(m):
        @pl.when(m + SLOTS < n_tiles)
        def _():
            start_tile(m + SLOTS)

    def wait_up_tile(slot):
        pltpu.make_async_copy(wg_hbm.at[0, :, pl.ds(0, TILE)], slots.at[slot, pl.ds(0, dim)], s_slot.at[slot, 0]).wait()

    def wait_down_pair(slot):
        for i in range(DOWN):
            pltpu.make_async_copy(wd_hbm.at[0, :, pl.ds(0, TILE)], slots.at[slot, pl.ds(i * ffn, ffn)], s_slot.at[slot, i]).wait()

    def swap(s, u, r, cols):
        return push(y.at[s, owner(r, 1 - core), u, :, cols], rb.at[r, u, :, cols], rs_ds.at[s, u, r], rs_dr.at[s, u, r], sibling)

    def swap_columns(s, u, first, size):
        if DO_COMM:
            for r in SWAP_ORDER:
                swap(s, u, r, columns(first, size)).start()

    def swapped(s, u, r):
        return swap(s, u, r, pl.ds(0, dim))

    def rs_right(s, u, k):
        r, hh = RS_RIGHT[k]
        return push(y.at[s, owner(r, core), u, rows(hh)], ring_l.at[u, k], rs_sr.at[s, u, 0, k], rs_rl.at[s, u, k], right)

    def rs_left(s, u, k):
        r, hh = RS_LEFT[k]
        return push(y.at[s, owner(r, core), u, rows(hh)], ring_r.at[u, k], rs_sr.at[s, u, 1, k], rs_rr.at[s, u, k], left)

    def add_in(dst, src):
        step = min(1024, dim)

        def body(i, carry):
            cols = pl.ds(pl.multiple_of(i * step, step), step)
            dst[:, cols] = (dst[:, cols].astype(F32) + src[:, cols].astype(F32)).astype(BF16)
            return carry

        repeat(dim // step, body)

    def fold(s, u, r):
        swapped(s, u, r).wait_recv()
        add_in(y.at[s, owner(r, core), u], rb.at[r, u])

    def rs1(s, u):
        fold(s, u, 2)
        rs_right(s, u, 0).start()
        rs_left(s, u, 0).start()

    def rs2(s, u):
        fold(s, u, 1)
        rs_right(s, u, 1).start()
        fold(s, u, 3)
        rs_left(s, u, 1).start()

    def rs3(s, u):
        rs_right(s, u, 0).wait_recv()
        add_in(y.at[s, owner(1, core), u, rows(0)], ring_l.at[u, 0])
        rs_right(s, u, 2).start()
        rs_left(s, u, 0).wait_recv()
        add_in(y.at[s, owner(3, core), u, rows(1)], ring_r.at[u, 0])
        rs_left(s, u, 2).start()

    def rs4_wait(s, u):
        swapped(s, u, 0).wait_recv()
        for k in LATER:
            rs_right(s, u, k).wait_recv()
            rs_left(s, u, k).wait_recv()

    def rs_drain(s):
        for u in PAIR:
            for r in range(4):
                swapped(s, u, r).wait_send()
            for k in range(3):
                rs_right(s, u, k).wait_send()
                rs_left(s, u, k).wait_send()

    def norm_row(i):
        return norms_ref[i // 4, pl.ds(i % 4, 1)]

    def inv_rms(v):
        return lax.rsqrt(jnp.sum(v * v, axis=-1, keepdims=True) * (1.0 / dim) + NORM_EPS)

    def finish(s, u, post, has_next):
        def body(hh, carry):
            at = rows(hh)
            total = (y[s, me, u, at].astype(F32) + rb[0, u, at].astype(F32)
                     + ring_l[u, 2 - hh].astype(F32) + ring_r[u, 1 + hh].astype(F32))
            v = total.astype(BF16).astype(F32)
            x1 = (xs[s, u, at].astype(F32) + v * inv_rms(v) * (1.0 + norm_row(post))).astype(BF16)
            xs[s, u, at] = x1
            if has_next:
                w = x1.astype(F32)
                g[s, me, u, at] = (w * inv_rms(w) * (1.0 + norm_row(post + 1))).astype(BF16)
            return carry

        repeat(2, body)

    def ag_right(t, u, k, table=AG_RIGHT):
        r, hh = table[k]
        ref = g.at[t, owner(r, core), u, rows(hh)]
        return push(ref, ref, ag_sr.at[t, u, 0, k], ag_rl.at[t, u, k], right)

    def ag_left(t, u, k, table=AG_LEFT):
        r, hh = table[k]
        ref = g.at[t, owner(r, core), u, rows(hh)]
        return push(ref, ref, ag_sr.at[t, u, 1, k], ag_rr.at[t, u, k], left)

    def from_left(t, u, k):
        ag_right(t, u, k, AG_FROM_LEFT).wait_recv()

    def from_right(t, u, k):
        ag_left(t, u, k, AG_FROM_RIGHT).wait_recv()

    def ag_d2d(t, u, r, c):
        ref = g.at[t, owner(r, c), u]
        return push(ref, ref, ag_ds.at[t, u, r], ag_dr.at[t, u, r], sibling)

    def ag_out(t, u, k):
        ag_right(t, u, k).start()
        ag_left(t, u, k).start()

    def ag_gone(t, u, k):
        ag_right(t, u, k).wait_send()
        ag_left(t, u, k).wait_send()

    def ag1(t, u):
        for k in PAIR:
            ag_out(t, u, k)
        ag_d2d(t, u, 0, core).start()

    def ag2(t, u):
        from_left(t, u, 0)
        ag_right(t, u, 2).start()
        from_right(t, u, 0)
        ag_left(t, u, 2).start()

    def ag3(t, u):
        from_left(t, u, 1)
        ag_d2d(t, u, 3, core).start()
        from_right(t, u, 1)
        ag_d2d(t, u, 1, core).start()

    def ag4(t, u):
        from_left(t, u, 2)
        from_right(t, u, 2)
        ag_d2d(t, u, 2, core).start()

    def ag_own(t):
        for u in PAIR:
            ag_d2d(t, u, 0, 1 - core).wait_recv()

    def ag5(t, u):
        for r in (1, 3, 2):
            ag_d2d(t, u, r, 1 - core).wait_recv()

    def ag_drain(t, first):
        for u in PAIR:
            pl.when(jnp.logical_not(first))(lambda: ag_gone(t, u, 0))
            for k in LATER:
                ag_gone(t, u, k)
            for r in range(4):
                ag_d2d(t, u, r, core).wait_send()

    def rows_of(v):
        return v.reshape(chunk // 2, v.shape[-1])

    def rope(v, s, u):
        return v * rows_of(cos_ref[s, :, u]) + pltpu.roll(v, hd // 2, 1) * rows_of(sin_ref[s, :, u])

    def project_q(i, u, s):
        p = dot(rows_of(g[s, :, u]), wqkv[i])
        for hh in range(TILE // hd):
            rot = rope(p[:, hh * hd:(hh + 1) * hd], s, u).astype(BF16)
            q_sc[i * (TILE // hd) + hh, :, u] = rot.reshape(devices, half, hd)

    def project_kv(u, s):
        p = dot(rows_of(g[s, :, u]), wqkv[n_q])
        k = rope(p[:, :hd], s, u).astype(BF16).reshape(devices, half, hd)
        v = p[:, hd:].astype(BF16).reshape(devices, half, hd)
        for j in range(devices):
            at = pl.ds(past + (2 * j + u) * half, half)
            kbuf[at] = k[j]
            vbuf[at] = v[j]

    def fresh_out(s, l):
        return [pltpu.make_async_copy(buf.at[pl.ds(past, chunk)], out.at[l, s], s_kvo.at[i])
                for i, (buf, out) in enumerate(((kbuf, kn_hbm), (vbuf, vn_hbm)))]

    def scores(head, u, s, l):
        row = lax.broadcasted_iota(jnp.int32, (chunk // 2, SCORE_KEYS), 0)
        token = row + jnp.bitwise_and(row, -half) + u * half
        diff = lax.broadcasted_iota(jnp.int32, (chunk // 2, SCORE_KEYS), 1) - token
        oldest = jnp.where(l == 0, start_ref[s] - past, -past)
        q = rows_of(q_sc[head, :, u])
        top = None
        for kb in range((past + chunk) // SCORE_KEYS):
            first = kb * SCORE_KEYS
            cols = pl.ds(first, SCORE_KEYS)
            t = jnp.tanh(dot_nt(q, kbuf[cols]) * c1) * c2
            if past // 2 <= first < past:
                t = t + bias[s, :, cols]
            if first < chunk:
                t = jnp.where(diff > oldest - first, t, MASKED)
            if first >= past:
                t = jnp.where(diff <= past - first, t, MASKED)
            t_sc[:, cols] = t
            for i in range(SCORE_KEYS // hd):
                ti = t[:, i * hd:(i + 1) * hd]
                top = ti if top is None else jnp.maximum(top, ti)
        mx_sc[...] = top

    def weigh(head, u):
        mc = jnp.max(mx_sc[...], axis=-1, keepdims=True) + float((past + chunk).bit_length())
        mc = jnp.broadcast_to(mc, (chunk // 2, hd))
        n_kb = (past + chunk) // KEYS
        total = acc = None
        pvs = []
        for kb in range(n_kb):
            cols = pl.ds(kb * KEYS, KEYS)
            if kb >= DIST:
                mc = jnp.maximum(mc, jnp.minimum(pvs[kb - DIST], LOWEST))
            ps = []
            for i in range(KEYS // hd):
                pi = jnp.exp2(t_sc[:, pl.ds(kb * KEYS + i * hd, hd)] - mc)
                total = pi if total is None else total + pi
                ps.append(pi.astype(BF16))
            pv = dot(jnp.concatenate(ps, axis=1), vbuf[cols])
            pvs.append(pv)
            acc = pv if acc is None else acc + pv
        o = acc / jnp.sum(total, axis=-1, keepdims=True)
        o_sc[:, u, :, pl.ds(pl.multiple_of(head * hd, hd), hd)] = o.astype(BF16).reshape(devices, half, hd)

    def out_tile(i, u, s):
        cols = columns(i * out_step, out_step)
        y[s, :, u, :, cols] = dot(rows_of(o_sc[:, u]), wo[:, cols]).astype(BF16).reshape(devices, half, out_step)

    def gated(x, sa, sb):
        return (jax.nn.gelu(dot(x, slots[sa, pl.ds(0, dim)]), approximate=True) * dot(x, slots[sb, pl.ds(0, dim)])).astype(BF16)

    def up_half(jj, u, s, m0):
        m = m0 + 2 * jj
        h_sc[:, u, :, columns(jj * TILE, TILE)] = gated(rows_of(g[s, :, u]), m % SLOTS, (m + 1) % SLOTS).reshape(devices, half, TILE)

    def up_tile(jj, s, m0):
        m = m0 + 2 * jj
        wait_up_tile(m % SLOTS)
        wait_up_tile((m + 1) % SLOTS)
        h = gated(g[s].reshape(chunk, dim), m % SLOTS, (m + 1) % SLOTS)
        h_sc[:, :, :, columns(jj * TILE, TILE)] = h.reshape(devices, 2, half, TILE)
        next_tile(m)
        next_tile(m + 1)

    def down_pairs(n, count, s, m0, u=None):
        m = m0 + 2 * n_up + n
        for i in range(count):
            wait_down_pair((m + i) % SLOTS)
        for i in range(count * DOWN):
            cols = columns((n % n_pairs * DOWN + i) * TILE, TILE)
            w = slots[(m + i // DOWN) % SLOTS, pl.ds(i % DOWN * ffn, ffn)]
            if u is None:
                y[s, :, :, :, cols] = dot(h_sc[...].reshape(chunk, ffn), w).astype(BF16).reshape(devices, 2, half, TILE)
            else:
                y[s, :, u, :, cols] = dot(rows_of(h_sc[:, u]), w).astype(BF16).reshape(devices, half, TILE)
        for i in range(count):
            next_tile(m + i)

    def settle(t, u, post, gather):
        rs4_wait(t, u)

        @pl.when(gather)
        def _():
            finish(t, u, post, True)
            ag1(t, u)

        @pl.when(jnp.logical_not(gather))
        def _():
            finish(t, u, post, False)

    def events(t, post, reduce, early, gather):
        def onward():
            rs3(t, 0)
            pl.when(jnp.logical_not(early))(lambda: rs2(t, 1))

        def if_reduce(what):
            return lambda: pl.when(reduce)(what)

        def if_gather(f, u):
            return lambda: pl.when(gather)(lambda: f(t, u))

        return (if_reduce(onward), if_reduce(lambda: settle(t, 0, post, gather)), if_reduce(lambda: rs3(t, 1)),
                if_reduce(lambda: settle(t, 1, post, gather)),
                if_gather(ag2, 0), if_gather(ag3, 0), if_gather(ag2, 1), if_gather(ag3, 1), if_gather(ag4, 0))

    def at(step, low, high, early, plan, todo):
        if DO_COMM:
            for (soon, late), what in sorted(zip(plan, todo), key=lambda e: e[0][1]):
                if low <= soon < high or low <= late < high:
                    pl.when(step == jnp.where(early, soon, late))(what)

    def rest(early, plan, todo, last):
        for (soon, late), what in zip(plan, todo):
            if max(soon, late) >= last:
                pl.when(jnp.where(early, soon, late) >= last)(what)

    def att_phase(l, s):
        t = 1 - s
        reduce = (l > 0) | (s > 0)
        early = l == 0
        todo = events(t, 4 * l - 1 + 2 * s, reduce, early, l >= 0)
        n_proj = n_q + 1
        n_out = dim // out_step
        first_block = 2 * n_proj
        per_half = 2 * heads + n_out
        last = first_block + 2 * per_half
        if DO_COMPUTE:
            for c in att_weight_copies(l)[:-1]:
                pl.when(s == 0)(c.wait)
        if DO_COMM:
            ag5(s, 0)

        def proj(i, carry):
            if DO_COMPUTE:
                pl.when(i % n_proj < n_q)(lambda: project_q(i % n_proj, i // n_proj, s))
                pl.when(i % n_proj == n_q)(lambda: project_kv(i // n_proj, s))
            if DO_COMM:
                pl.when(i == 0)(lambda: ag4(s, 1))

                @pl.when(i == n_proj - 1)
                def _():
                    ag5(s, 1)
                    ag_drain(s, (l == 0) & (s == 0))
            at(i, 0, first_block, early, ATT_PLAN, todo)
            return carry

        repeat(first_block, proj)
        if DO_COMPUTE:
            for c in fresh_out(s, l):
                c.start()
            for c in cache_copies(kl_hbm, vl_hbm, s):
                c.wait()
        for u in PAIR:
            low = first_block + u * per_half

            def blk(i, carry):
                if DO_COMPUTE:
                    pl.when(i % 2 == 0)(lambda: scores(i // 2, u, s, l))
                    pl.when(i % 2 == 1)(lambda: weigh(i // 2, u))
                at(low + i, low, low + 2 * heads, early, ATT_PLAN, todo)
                if DO_COMM and u == 1:
                    @pl.when(early & (i == 1))
                    def _():
                        ag_own(t)
                        swap_columns(s, 0, 0, dim)

                    @pl.when(early & (i == LEAVE))
                    def _():
                        rs1(s, 0)
                        rs2(s, 0)
                return carry

            repeat(2 * heads, blk)
            if DO_COMPUTE and u == 0:
                pl.when(s == 0)(att_weight_copies(l)[-1].wait)
            if DO_COMPUTE and u == 1:
                for c in fresh_out(s, l):
                    c.wait()

                @pl.when((l == 0) & (s == 0))
                def _():
                    for c in cache_copies(kl_hbm, vl_hbm, 1):
                        c.start()

                @pl.when(l + s == 1)
                def _():
                    for c in cache_copies(kg_hbm, vg_hbm, l):
                        c.start()
            if DO_COMM:
                if u == 1:
                    pl.when(jnp.logical_not(early))(lambda: ag_own(t))

            def out_body(i, carry):
                if DO_COMPUTE:
                    out_tile(i, u, s)
                for j in range(out_step // swap_step):
                    first = i * out_step + j * swap_step
                    if u == 1:
                        pl.when(jnp.logical_not(early))(lambda: swap_columns(s, 0, first, swap_step))
                        swap_columns(s, 1, first, swap_step)
                at(low + 2 * heads + i, low + 2 * heads, low + per_half, early, ATT_PLAN, todo)
                return carry

            repeat(n_out, out_body)
        if DO_COMPUTE:
            @pl.when((s == 1) & (l == 0))
            def _():
                for c in att_weight_copies(1):
                    c.start()
        if DO_COMM:
            @pl.when(early)
            def _():
                rs1(s, 1)
                rs2(s, 1)

            @pl.when(jnp.logical_not(early))
            def _():
                rs1(s, 0)
                rs2(s, 0)
                rs1(s, 1)
            rest(early, ATT_PLAN, todo, last)
            pl.when(reduce)(lambda: rs_drain(t))

    def mlp_phase(l, s):
        t = 1 - s
        m0 = (2 * l + s) * per_phase
        gather = (l == 0) | (s == 0)
        early = l + s == 0
        todo = events(t, 4 * l + 1 + 2 * s, l >= 0, early, gather)
        first_down = n_up + 2
        last = first_down + n_pairs
        if DO_COMM:
            ag5(s, 0)

        def halves(i, carry):
            if DO_COMPUTE:
                m = m0 + 2 * i

                @pl.when(i < 2)
                def _():
                    wait_up_tile(m % SLOTS)
                    wait_up_tile((m + 1) % SLOTS)
                up_half(i % 2, i // 2, s, m0)

                @pl.when(i >= 2)
                def _():
                    next_tile(m - 4)
                    next_tile(m - 3)
            if DO_COMM:
                pl.when(i == 0)(lambda: ag4(s, 1))

                @pl.when(i == 1)
                def _():
                    ag5(s, 1)
                    ag_drain(s, l < 0)
            at(i, 0, 4, early, MLP_PLAN, todo)
            return carry

        repeat(4, halves)

        def ups(jj, carry):
            if DO_COMPUTE:
                up_tile(jj, s, m0)
            at(2 + jj, 4, first_down, early, MLP_PLAN, todo)
            return carry

        repeat(n_up, ups, 2)

        every = swap_step // (DOWN * TILE)

        @pl.when(gather)
        def _():
            def downs(n, carry):
                if DO_COMPUTE:
                    down_pairs(n, 1, s, m0)
                if DO_COMM:
                    pl.when(n == every - 1)(lambda: ag_own(t))

                @pl.when(n % every == every - 1)
                def _():
                    for u in PAIR:
                        swap_columns(s, u, n // every * swap_step, swap_step)
                at(first_down + n, first_down, last, early, MLP_PLAN, todo)
                return carry

            repeat(n_pairs, downs)
            if DO_COMM:
                rs1(s, 0)
                rs2(s, 0)
                rs1(s, 1)
                rest(early, MLP_PLAN, todo, last)

        @pl.when(jnp.logical_not(gather))
        def _():
            if DO_COMM:
                rest(early, MLP_PLAN[:4], todo, first_down)
                for dev in partners:
                    pl.semaphore_signal(credit, inc=1, device_id=dev, device_id_type=MESH_ID)
            n_steps = n_pairs // GROUP
            rare = max(n_steps // 2, 1)
            width = rare * GROUP * DOWN * TILE
            for u in PAIR:
                def downs(n, carry):
                    if DO_COMPUTE:
                        down_pairs(u * n_pairs + n * GROUP, GROUP, s, m0, u)
                    if DO_COMM:
                        if u == 0:
                            pl.when(n == rare - 1)(lambda: pl.semaphore_wait(credit, len(partners)))
                        pl.when(n % rare == rare - 1)(lambda: swap_columns(s, u, n // rare * width, width))
                        if u == 1:
                            @pl.when(n == 0)
                            def _():
                                rs1(s, 0)
                                rs2(s, 0)
                    return carry

                repeat(n_steps, downs)
            if DO_COMM:
                rs1(s, 1)
                rs3(s, 0)
                fold(s, 1, 1)
                fold(s, 1, 3)
                pl.delay(HOLD_NS)
                rs_right(s, 1, 1).start()
                rs_left(s, 1, 1).start()
        if DO_COMM:
            rs_drain(t)

    first = [pltpu.make_async_copy(src, dst, s_x.at[i]) for i, (src, dst) in enumerate(((x_hbm, xs), (norms_hbm, norms_ref), (freq_hbm, freq_ref)))]
    for copy in first:
        copy.start()
    barrier = pltpu.get_barrier_semaphore()
    for dev in partners:
        pl.semaphore_signal(barrier, inc=1, device_id=dev, device_id_type=MESH_ID)

    def first_norm(s, u):
        def body(hh, carry):
            v = xs[s, u, rows(hh)].astype(F32)
            g[s, me, u, rows(hh)] = (v * inv_rms(v) * (1.0 + norm_row(0))).astype(BF16)
            return carry

        repeat(2, body)

    for copy in first:
        copy.wait()
    first_norm(0, 0)
    pl.semaphore_wait(barrier, len(partners))
    for u in PAIR:
        if u == 1:
            first_norm(0, 1)
        if DO_COMM:
            ag_out(0, u, 0)
            ag_d2d(0, u, 0, core).start()
    if DO_COMPUTE:
        for c in att_weight_copies(0) + cache_copies(kl_hbm, vl_hbm, 0):
            c.start()
        for m in range(SLOTS):
            start_tile(jnp.int32(m))
    for u in PAIR:
        first_norm(1, u)
    for s in PAIR:
        shape = cos_ref.shape[1:]
        pos = start_ref[s] + sum(n * lax.broadcasted_iota(jnp.int32, shape, i) for i, n in enumerate((2 * half, half, 1)))
        angle = pos.astype(F32) * freq_ref[...]
        cos_ref[s] = jnp.cos(angle)
        sin = jnp.sin(angle)
        sin_ref[s] = jnp.where(lax.broadcasted_iota(jnp.int32, shape, 3) < hd // 2, -sin, sin)
        bias[s] = jnp.where(lax.broadcasted_iota(jnp.int32, (1, past), 1) < start_ref[s], 0.0, MASKED)
    if DO_COMM:
        for u in PAIR:
            ag_gone(0, u, 0)
            ag_out(0, u, 1)
        for u in PAIR:
            ag2(0, u)
        for u in PAIR:
            ag3(0, u)
        ag4(0, 0)
        ag_own(0)
        for u in PAIR:
            ag1(1, u)

    def layer(l, carry):
        def att(s, carry):
            att_phase(l, s)
            return carry

        def mlp(s, carry):
            mlp_phase(l, s)
            return carry

        repeat(2, att)
        repeat(2, mlp)
        return carry

    repeat(2, layer)

    out = [pltpu.make_async_copy(xs.at[s, u], xo_hbm.at[s, u], s_xo.at[s, u]) for s in PAIR for u in PAIR]
    out[0].start()
    out[1].start()
    for u in PAIR:
        if DO_COMM:
            if u == 1:
                rs3(1, 1)
            rs4_wait(1, u)
            finish(1, u, 7, False)
        out[2 + u].start()
    if DO_COMM:
        rs_drain(1)
    for copy in out:
        copy.wait()


def run_layers(x, start, freq, norms, kl, vl, kg, vg, wq, wk, wv, wo, wg, wu, wd):
    seqs, _, half, dim = x.shape
    _, past, hd = kl.shape
    chunk = kg.shape[1] - past
    n_q = wq.shape[2] // TILE
    devices = chunk // (2 * half)
    ring = pltpu.VMEM((2, 3, half // 2, dim), BF16)
    keys = pltpu.VMEM((past + chunk, hd), BF16)
    whole = pltpu.VMEM((2, devices, 2, half, dim), BF16)
    table = pltpu.VMEM((2, devices, 2, half, hd), F32)

    def dmas(*shape):
        return pltpu.SemaphoreType.DMA(shape)

    scratch = [
        whole, whole,
        pltpu.VMEM((4, 2, half, dim), BF16),
        ring, ring,
        pltpu.VMEM(x.shape, BF16),
        pltpu.VMEM(norms.shape, F32), pltpu.VMEM(freq.shape, F32),
        table, table,
        pltpu.VMEM((2, 1, past), F32),
        pltpu.VMEM((n_q + 1, dim, TILE), BF16),
        pltpu.VMEM(wo.shape[1:], BF16),
        pltpu.VMEM((SLOTS, max(dim, DOWN * wd.shape[1]), TILE), BF16),
        pltpu.VMEM((devices, 2, half, wg.shape[2]), BF16),
        pltpu.VMEM((wq.shape[2] // hd, devices, 2, half, hd), BF16),
        pltpu.VMEM((devices, 2, half, wq.shape[2]), BF16),
        keys, keys,
        pltpu.VMEM((chunk // 2, past + chunk), F32),
        pltpu.VMEM((chunk // 2, hd), F32),
        dmas(3), dmas(n_q + 3), dmas(SLOTS, DOWN), dmas(2), dmas(2), dmas(2, 2), pltpu.SemaphoreType.REGULAR,
    ]
    chips = [dmas(2, 2, 3)] * 2
    cores = [dmas(2, 2, 4)] * 2
    sends = [dmas(2, 2, 2, 3)]
    scratch += cores + chips + sends + sends + chips + cores
    return pl.pallas_call(
        layers_kernel,
        out_shape=(jax.ShapeDtypeStruct(x.shape, BF16),) + (jax.ShapeDtypeStruct((2, seqs, chunk, hd), BF16),) * 2,
        in_specs=[ANY, SMEM] + [ANY] * 13,
        out_specs=(ANY,) * 3,
        scratch_shapes=scratch,
        compiler_params=pltpu.CompilerParams(collective_id=0, has_side_effects=True, vmem_limit_bytes=LAYERS_LIMIT),
        name='layers',
    )(x, start, freq, norms, kl, vl, kg, vg, wq, wk, wv, wo, wg, wu, wd)


def cache_kernel(start_ref, x, k_new, v_new, kl, vl, kg, vg, x_o, kl_o, vl_o, kg_o, vg_o, xbuf, buf, fresh, turned, s_x, s_in, s_fr, s_out):
    _, _, chunk, _ = k_new.shape
    _, window, _ = kl.shape
    _, size, hd = fresh.shape
    lead = size - chunk
    jobs = []
    for b in PAIR:
        for l, group in enumerate((((kl, k_new, kl_o), (vl, v_new, vl_o)), ((kg, k_new, kg_o), (vg, v_new, vg_o)))):
            jobs += [(c, new, out, l, b) for c, new, out in group]
    rows_in = [pltpu.make_async_copy(new.at[l, b], fresh.at[i, pl.ds(0, chunk)], s_fr.at[i]) for i, (_, new, _, l, b) in enumerate(jobs)]
    loads = [pltpu.make_async_copy(c.at[b], buf.at[i, pl.ds(0, c.shape[1])], s_in.at[i]) for i, (c, _, _, _, b) in enumerate(jobs)]
    stores = [pltpu.make_async_copy(buf.at[i, pl.ds(0, c.shape[1])], out.at[b], s_out.at[i]) for i, (c, _, out, _, b) in enumerate(jobs)]
    x_in = pltpu.make_async_copy(x, xbuf, s_x)
    x_out = pltpu.make_async_copy(xbuf, x_o, s_x)
    for copy in rows_in + loads + [x_in]:
        copy.start()
    for i, (_, _, _, l, b) in enumerate(jobs):
        rows_in[i].wait()
        turned[i] = pltpu.roll(fresh[i].astype(F32), start_ref[b] % lead, 0).astype(BF16)
    row = lax.broadcasted_iota(jnp.int32, (lead, hd), 0)
    for i, (_, _, _, l, b) in enumerate(jobs):
        loads[i].wait()
        start = start_ref[b]
        r = start % lead
        at = pl.multiple_of(start - r, lead)
        end = pl.ds(pl.multiple_of(at + chunk, lead), lead)
        first = buf[i, pl.ds(at, lead)].astype(F32)
        after = buf[i, end].astype(F32)
        buf[i, pl.ds(at, lead)] = jnp.where(row >= r, turned[i, pl.ds(0, lead)].astype(F32), first).astype(BF16)
        buf[i, pl.ds(pl.multiple_of(at + lead, lead), chunk - lead)] = turned[i, pl.ds(lead, chunk - lead)]
        buf[i, end] = jnp.where(row < r, turned[i, pl.ds(chunk, lead)].astype(F32), after).astype(BF16)
        if l == 0:
            over = buf[i, pl.ds(window, chunk)].astype(F32)
            head = buf[i, pl.ds(0, chunk)].astype(F32)
            landed = lax.broadcasted_iota(jnp.int32, over.shape, 0) < start + chunk - window
            buf[i, pl.ds(0, chunk)] = jnp.where(landed, over, head).astype(BF16)
        stores[i].start()
    x_in.wait()
    x_out.start()
    for copy in stores + [x_out]:
        copy.wait()


def write_caches(start, x, k_new, v_new, kl, vl, kg, vg):
    _, _, hd = kl.shape
    _, _, chunk, _ = k_new.shape
    lead = 16
    depth = max(kl.shape[1] + chunk, kg.shape[1]) + lead
    jobs = 4 * len(PAIR)
    dmas = pltpu.SemaphoreType.DMA((jobs,))
    chunks = pltpu.VMEM((jobs, chunk + lead, hd), BF16)
    return pl.pallas_call(
        cache_kernel,
        out_shape=tuple(jax.ShapeDtypeStruct(c.shape, BF16) for c in (x, kl, vl, kg, vg)),
        in_specs=[SMEM] + [ANY] * 7,
        out_specs=(ANY,) * 5,
        scratch_shapes=[pltpu.VMEM(x.shape, BF16), pltpu.VMEM((jobs, depth, hd), BF16), chunks, chunks,
                        pltpu.SemaphoreType.DMA, dmas, dmas, dmas],
        compiler_params=pltpu.CompilerParams(vmem_limit_bytes=VMEM_LIMIT),
        name='write_caches',
    )(start, x, k_new, v_new, kl, vl, kg, vg)


def solution(mesh):
    act_spec = P('dp', 'tp', None)
    cache_spec = P('dp', None, 'tp', None)
    col_spec = P(None, None, 'tp')
    row_spec = P(None, 'tp', None)
    arg_specs = (act_spec, P('dp'), cache_spec, cache_spec, cache_spec, cache_spec, P(), col_spec, col_spec, col_spec, row_spec, col_spec, col_spec, row_spec)
    result_specs = (act_spec, cache_spec, cache_spec, cache_spec, cache_spec)

    def device_step(x, start, k_local, v_local, k_global, v_global, norms, w_q, w_k, w_v, w_o, w_gate, w_up, w_down):
        hd = k_local.shape[3]
        freq = ROPE_BASE ** (np.arange(hd // 2) * (-2.0 / hd))
        freq = jnp.asarray(np.concatenate([freq, freq])[None], F32)
        flat = [c.reshape(c.shape[0], c.shape[1], hd) for c in (k_local, v_local, k_global, v_global)]
        x4 = x.reshape(x.shape[0], 2, x.shape[1] // 2, x.shape[2])
        x_out, k_new, v_new = run_layers(x4, start, freq, norms, *flat, w_q, w_k, w_v, w_o, w_gate, w_up, w_down)
        x_out = x_out.reshape(x.shape)
        x_out, *caches = write_caches(start, x_out, k_new, v_new, *flat)
        return (x_out,) + tuple(c.reshape(c.shape[0], c.shape[1], 1, hd) for c in caches)

    return jax.shard_map(device_step, mesh=mesh, in_specs=arg_specs, out_specs=result_specs, check_vma=False)
```

```python
import jax
import jax.numpy as jnp
import numpy as np
from jax import lax
from jax.experimental import pallas as pl
from jax.experimental.pallas import tpu as pltpu
from jax.sharding import PartitionSpec as P

SOFT_CAP = 50.0
NORM_EPS = 1e-6
ROPE_BASE = 10000.0
MASKED = -1e30
DIST = 2
LOWEST = -3e38
LOG2E = 1.4426950408889634

BF16 = jnp.bfloat16
F32 = jnp.float32
MESH_ID = pl.DeviceIdType.MESH
ANY = pl.BlockSpec(memory_space=pl.ANY)
VMEM = pl.BlockSpec(memory_space=pltpu.VMEM)
SMEM = pl.BlockSpec(memory_space=pltpu.SMEM)

TILE = 256
SLOTS = 6
DOWN = 2
SCORE_KEYS = 256
KEYS = 512
OUT = 2048
VMEM_LIMIT = 67_000_000
LAYERS_LIMIT = 67_000_000
SWAP = 1024
ATT_PLAN = ((2, 4), (10, 11), (7, 9), (14, 17), (14, 19), (18, 21), (19, 23), (21, 24), (24, 26))
MLP_PLAN = ((1, 2), (6, 6), (4, 5), (8, 8), (9, 10), (11, 11), (13, 13), (15, 15), (16, 16))
LEAVE = 4
GROUP = 2
HOLD_NS = 1000
SWAP_ORDER = (2, 1, 3, 0)
DO_COMPUTE = True
DO_COMM = True

PAIR = range(2)
LATER = (1, 2)


def mirror(table):
    return tuple(((4 - r) % 4, 1 - hh) for r, hh in table)


RS_RIGHT = ((2, 0), (1, 1), (1, 0))
RS_LEFT = mirror(RS_RIGHT)
AG_RIGHT = ((0, 0), (0, 1), (3, 0))
AG_LEFT = mirror(AG_RIGHT)
AG_FROM_LEFT = ((3, 0), (3, 1), (2, 0))
AG_FROM_RIGHT = mirror(AG_FROM_LEFT)


def repeat(n, body, low=0):
    lax.fori_loop(low, n, body, 0)


def dot(a, b):
    return jnp.dot(a, b, preferred_element_type=F32)


def dot_nt(a, b):
    return lax.dot_general(a, b, (((1,), (1,)), ((), ())), preferred_element_type=F32)


def layers_kernel(x_hbm, start_ref, freq_hbm, norms_hbm, kl_hbm, vl_hbm, kg_hbm, vg_hbm,
                  wq_hbm, wk_hbm, wv_hbm, wo_hbm, wg_hbm, wu_hbm, wd_hbm,
                  xo_hbm, kn_hbm, vn_hbm,
                  g, y, rb, ring_l, ring_r, xs, norms_ref, freq_ref, cos_ref, sin_ref, bias, wqkv, wo, slots, h_sc, q_sc, o_sc, kbuf, vbuf, t_sc, mx_sc,
                  s_x, s_attw, s_slot, s_kv, s_kvo, s_xo, credit,
                  rs_ds, rs_dr, rs_rl, rs_rr, rs_sr, ag_sr, ag_rl, ag_rr, ag_ds, ag_dr):
    _, devices, _, half, dim = g.shape
    chunk = devices * 2 * half
    piece = half // 2
    keys, hd = kbuf.shape
    past = keys - chunk
    n_q = wq_hbm.shape[2] // TILE
    heads = wq_hbm.shape[2] // hd
    ffn = wg_hbm.shape[2]
    n_up = ffn // TILE
    n_down = dim // TILE
    n_pairs = n_down // DOWN
    per_phase = 2 * n_up + n_pairs
    n_tiles = 4 * per_phase + n_pairs
    out_step = min(OUT, dim)
    swap_step = min(SWAP, dim)
    c1 = (hd ** -0.5) / SOFT_CAP
    c2 = SOFT_CAP * LOG2E

    dp = lax.axis_index('dp')
    me = lax.axis_index('tp')
    chip = me // 2
    core = me % 2
    chips = devices // 2
    right = (dp, (chip + 1) % chips * 2 + core)
    left = (dp, (chip + chips - 1) % chips * 2 + core)
    sibling = (dp, chip * 2 + 1 - core)
    partners = (sibling, left, right)

    def owner(offset, c):
        return (chip + offset) % chips * 2 + c

    def columns(first, size):
        return pl.ds(pl.multiple_of(first, TILE), size)

    def rows(hh):
        return pl.ds(pl.multiple_of(hh * piece, piece), piece)

    def push(src, dst, ssem, rsem, dev):
        return pltpu.make_async_remote_copy(src_ref=src, dst_ref=dst, send_sem=ssem, recv_sem=rsem, device_id=dev, device_id_type=MESH_ID)

    def att_weight_copies(l):
        out = [pltpu.make_async_copy(wq_hbm.at[l, :, pl.ds(i * TILE, TILE)], wqkv.at[i], s_attw.at[i]) for i in range(n_q)]
        out.append(pltpu.make_async_copy(wk_hbm.at[l], wqkv.at[n_q, :, pl.ds(0, hd)], s_attw.at[n_q]))
        out.append(pltpu.make_async_copy(wv_hbm.at[l], wqkv.at[n_q, :, pl.ds(hd, hd)], s_attw.at[n_q + 1]))
        out.append(pltpu.make_async_copy(wo_hbm.at[l], wo, s_attw.at[n_q + 2]))
        return out

    def cache_copies(k_hbm, v_hbm, s):
        return [pltpu.make_async_copy(c.at[s, pl.ds(0, past)], buf.at[pl.ds(0, past)], s_kv.at[i])
                for i, (c, buf) in enumerate(((k_hbm, kbuf), (v_hbm, vbuf)))]

    def start_tile(m):
        slot = m % SLOTS
        m = jnp.where(m < n_tiles - n_pairs, m, m - n_pairs)
        layer = m // (2 * per_phase)
        j = m % per_phase

        @pl.when((j < 2 * n_up) & (j % 2 == 0))
        def _():
            pltpu.make_async_copy(wg_hbm.at[layer, :, columns(j // 2 * TILE, TILE)], slots.at[slot, pl.ds(0, dim)], s_slot.at[slot, 0]).start()

        @pl.when((j < 2 * n_up) & (j % 2 == 1))
        def _():
            pltpu.make_async_copy(wu_hbm.at[layer, :, columns(j // 2 * TILE, TILE)], slots.at[slot, pl.ds(0, dim)], s_slot.at[slot, 0]).start()

        @pl.when(j >= 2 * n_up)
        def _():
            for i in range(DOWN):
                pltpu.make_async_copy(wd_hbm.at[layer, :, columns(((j - 2 * n_up) * DOWN + i) * TILE, TILE)],
                                      slots.at[slot, pl.ds(i * ffn, ffn)], s_slot.at[slot, i]).start()

    def next_tile(m):
        @pl.when(m + SLOTS < n_tiles)
        def _():
            start_tile(m + SLOTS)

    def wait_up_tile(slot):
        pltpu.make_async_copy(wg_hbm.at[0, :, pl.ds(0, TILE)], slots.at[slot, pl.ds(0, dim)], s_slot.at[slot, 0]).wait()

    def wait_down_pair(slot):
        for i in range(DOWN):
            pltpu.make_async_copy(wd_hbm.at[0, :, pl.ds(0, TILE)], slots.at[slot, pl.ds(i * ffn, ffn)], s_slot.at[slot, i]).wait()

    def swap(s, u, r, cols):
        return push(y.at[s, owner(r, 1 - core), u, :, cols], rb.at[r, u, :, cols], rs_ds.at[s, u, r], rs_dr.at[s, u, r], sibling)

    def swap_columns(s, u, first, size):
        if DO_COMM:
            for r in SWAP_ORDER:
                swap(s, u, r, columns(first, size)).start()

    def swapped(s, u, r):
        return swap(s, u, r, pl.ds(0, dim))

    def rs_right(s, u, k):
        r, hh = RS_RIGHT[k]
        return push(y.at[s, owner(r, core), u, rows(hh)], ring_l.at[u, k], rs_sr.at[s, u, 0, k], rs_rl.at[s, u, k], right)

    def rs_left(s, u, k):
        r, hh = RS_LEFT[k]
        return push(y.at[s, owner(r, core), u, rows(hh)], ring_r.at[u, k], rs_sr.at[s, u, 1, k], rs_rr.at[s, u, k], left)

    def add_in(dst, src):
        step = min(1024, dim)

        def body(i, carry):
            cols = pl.ds(pl.multiple_of(i * step, step), step)
            dst[:, cols] = (dst[:, cols].astype(F32) + src[:, cols].astype(F32)).astype(BF16)
            return carry

        repeat(dim // step, body)

    def fold(s, u, r):
        swapped(s, u, r).wait_recv()
        add_in(y.at[s, owner(r, core), u], rb.at[r, u])

    def rs1(s, u):
        fold(s, u, 2)
        rs_right(s, u, 0).start()
        rs_left(s, u, 0).start()

    def rs2(s, u):
        fold(s, u, 1)
        rs_right(s, u, 1).start()
        fold(s, u, 3)
        rs_left(s, u, 1).start()

    def rs3(s, u):
        rs_right(s, u, 0).wait_recv()
        add_in(y.at[s, owner(1, core), u, rows(0)], ring_l.at[u, 0])
        rs_right(s, u, 2).start()
        rs_left(s, u, 0).wait_recv()
        add_in(y.at[s, owner(3, core), u, rows(1)], ring_r.at[u, 0])
        rs_left(s, u, 2).start()

    def rs4_wait(s, u):
        swapped(s, u, 0).wait_recv()
        for k in LATER:
            rs_right(s, u, k).wait_recv()
            rs_left(s, u, k).wait_recv()

    def rs_drain(s):
        for u in PAIR:
            for r in range(4):
                swapped(s, u, r).wait_send()
            for k in range(3):
                rs_right(s, u, k).wait_send()
                rs_left(s, u, k).wait_send()

    def norm_row(i):
        return norms_ref[i // 4, pl.ds(i % 4, 1)]

    def inv_rms(v):
        return lax.rsqrt(jnp.sum(v * v, axis=-1, keepdims=True) * (1.0 / dim) + NORM_EPS)

    def finish(s, u, post, has_next):
        def body(hh, carry):
            at = rows(hh)
            total = (y[s, me, u, at].astype(F32) + rb[0, u, at].astype(F32)
                     + ring_l[u, 2 - hh].astype(F32) + ring_r[u, 1 + hh].astype(F32))
            v = total.astype(BF16).astype(F32)
            x1 = (xs[s, u, at].astype(F32) + v * inv_rms(v) * (1.0 + norm_row(post))).astype(BF16)
            xs[s, u, at] = x1
            if has_next:
                w = x1.astype(F32)
                g[s, me, u, at] = (w * inv_rms(w) * (1.0 + norm_row(post + 1))).astype(BF16)
            return carry

        repeat(2, body)

    def ag_right(t, u, k, table=AG_RIGHT):
        r, hh = table[k]
        ref = g.at[t, owner(r, core), u, rows(hh)]
        return push(ref, ref, ag_sr.at[t, u, 0, k], ag_rl.at[t, u, k], right)

    def ag_left(t, u, k, table=AG_LEFT):
        r, hh = table[k]
        ref = g.at[t, owner(r, core), u, rows(hh)]
        return push(ref, ref, ag_sr.at[t, u, 1, k], ag_rr.at[t, u, k], left)

    def from_left(t, u, k):
        ag_right(t, u, k, AG_FROM_LEFT).wait_recv()

    def from_right(t, u, k):
        ag_left(t, u, k, AG_FROM_RIGHT).wait_recv()

    def ag_d2d(t, u, r, c):
        ref = g.at[t, owner(r, c), u]
        return push(ref, ref, ag_ds.at[t, u, r], ag_dr.at[t, u, r], sibling)

    def ag_out(t, u, k):
        ag_right(t, u, k).start()
        ag_left(t, u, k).start()

    def ag_gone(t, u, k):
        ag_right(t, u, k).wait_send()
        ag_left(t, u, k).wait_send()

    def ag1(t, u):
        for k in PAIR:
            ag_out(t, u, k)
        ag_d2d(t, u, 0, core).start()

    def ag2(t, u):
        from_left(t, u, 0)
        ag_right(t, u, 2).start()
        from_right(t, u, 0)
        ag_left(t, u, 2).start()

    def ag3(t, u):
        from_left(t, u, 1)
        ag_d2d(t, u, 3, core).start()
        from_right(t, u, 1)
        ag_d2d(t, u, 1, core).start()

    def ag4(t, u):
        from_left(t, u, 2)
        from_right(t, u, 2)
        ag_d2d(t, u, 2, core).start()

    def ag_own(t):
        for u in PAIR:
            ag_d2d(t, u, 0, 1 - core).wait_recv()

    def ag5(t, u):
        for r in (1, 3, 2):
            ag_d2d(t, u, r, 1 - core).wait_recv()

    def ag_drain(t, first):
        for u in PAIR:
            pl.when(jnp.logical_not(first))(lambda: ag_gone(t, u, 0))
            for k in LATER:
                ag_gone(t, u, k)
            for r in range(4):
                ag_d2d(t, u, r, core).wait_send()

    def rows_of(v):
        return v.reshape(chunk // 2, v.shape[-1])

    def rope(v, s, u):
        return v * rows_of(cos_ref[s, :, u]) + pltpu.roll(v, hd // 2, 1) * rows_of(sin_ref[s, :, u])

    def project_q(i, u, s):
        p = dot(rows_of(g[s, :, u]), wqkv[i])
        for hh in range(TILE // hd):
            rot = rope(p[:, hh * hd:(hh + 1) * hd], s, u).astype(BF16)
            q_sc[i * (TILE // hd) + hh, :, u] = rot.reshape(devices, half, hd)

    def project_kv(u, s):
        p = dot(rows_of(g[s, :, u]), wqkv[n_q])
        k = rope(p[:, :hd], s, u).astype(BF16).reshape(devices, half, hd)
        v = p[:, hd:].astype(BF16).reshape(devices, half, hd)
        for j in range(devices):
            at = pl.ds(past + (2 * j + u) * half, half)
            kbuf[at] = k[j]
            vbuf[at] = v[j]

    def fresh_out(s, l):
        return [pltpu.make_async_copy(buf.at[pl.ds(past, chunk)], out.at[l, s], s_kvo.at[i])
                for i, (buf, out) in enumerate(((kbuf, kn_hbm), (vbuf, vn_hbm)))]

    def scores(head, u, s, l):
        row = lax.broadcasted_iota(jnp.int32, (chunk // 2, SCORE_KEYS), 0)
        token = row + jnp.bitwise_and(row, -half) + u * half
        diff = lax.broadcasted_iota(jnp.int32, (chunk // 2, SCORE_KEYS), 1) - token
        oldest = jnp.where(l == 0, start_ref[s] - past, -past)
        q = rows_of(q_sc[head, :, u])
        top = None
        for kb in range((past + chunk) // SCORE_KEYS):
            first = kb * SCORE_KEYS
            cols = pl.ds(first, SCORE_KEYS)
            t = jnp.tanh(dot_nt(q, kbuf[cols]) * c1) * c2
            if past // 2 <= first < past:
                t = t + bias[s, :, cols]
            if first < chunk:
                t = jnp.where(diff > oldest - first, t, MASKED)
            if first >= past:
                t = jnp.where(diff <= past - first, t, MASKED)
            t_sc[:, cols] = t
            for i in range(SCORE_KEYS // hd):
                ti = t[:, i * hd:(i + 1) * hd]
                top = ti if top is None else jnp.maximum(top, ti)
        mx_sc[...] = top

    def weigh(head, u):
        mc = jnp.max(mx_sc[...], axis=-1, keepdims=True) + float((past + chunk).bit_length())
        mc = jnp.broadcast_to(mc, (chunk // 2, hd))
        n_kb = (past + chunk) // KEYS
        total = acc = None
        pvs = []
        for kb in range(n_kb):
            cols = pl.ds(kb * KEYS, KEYS)
            if kb >= DIST:
                mc = jnp.maximum(mc, jnp.minimum(pvs[kb - DIST], LOWEST))
            ps = []
            for i in range(KEYS // hd):
                pi = jnp.exp2(t_sc[:, pl.ds(kb * KEYS + i * hd, hd)] - mc)
                total = pi if total is None else total + pi
                ps.append(pi.astype(BF16))
            pv = dot(jnp.concatenate(ps, axis=1), vbuf[cols])
            pvs.append(pv)
            acc = pv if acc is None else acc + pv
        o = acc / jnp.sum(total, axis=-1, keepdims=True)
        o_sc[:, u, :, pl.ds(pl.multiple_of(head * hd, hd), hd)] = o.astype(BF16).reshape(devices, half, hd)

    def out_tile(i, u, s):
        cols = columns(i * out_step, out_step)
        y[s, :, u, :, cols] = dot(rows_of(o_sc[:, u]), wo[:, cols]).astype(BF16).reshape(devices, half, out_step)

    def gated(x, sa, sb):
        return (jax.nn.gelu(dot(x, slots[sa, pl.ds(0, dim)]), approximate=True) * dot(x, slots[sb, pl.ds(0, dim)])).astype(BF16)

    def up_half(jj, u, s, m0):
        m = m0 + 2 * jj
        h_sc[:, u, :, columns(jj * TILE, TILE)] = gated(rows_of(g[s, :, u]), m % SLOTS, (m + 1) % SLOTS).reshape(devices, half, TILE)

    def up_tile(jj, s, m0):
        m = m0 + 2 * jj
        wait_up_tile(m % SLOTS)
        wait_up_tile((m + 1) % SLOTS)
        h = gated(g[s].reshape(chunk, dim), m % SLOTS, (m + 1) % SLOTS)
        h_sc[:, :, :, columns(jj * TILE, TILE)] = h.reshape(devices, 2, half, TILE)
        next_tile(m)
        next_tile(m + 1)

    def down_pairs(n, count, s, m0, u=None):
        m = m0 + 2 * n_up + n
        for i in range(count):
            wait_down_pair((m + i) % SLOTS)
        for i in range(count * DOWN):
            cols = columns((n % n_pairs * DOWN + i) * TILE, TILE)
            w = slots[(m + i // DOWN) % SLOTS, pl.ds(i % DOWN * ffn, ffn)]
            if u is None:
                y[s, :, :, :, cols] = dot(h_sc[...].reshape(chunk, ffn), w).astype(BF16).reshape(devices, 2, half, TILE)
            else:
                y[s, :, u, :, cols] = dot(rows_of(h_sc[:, u]), w).astype(BF16).reshape(devices, half, TILE)
        for i in range(count):
            next_tile(m + i)

    def settle(t, u, post, gather):
        rs4_wait(t, u)

        @pl.when(gather)
        def _():
            finish(t, u, post, True)
            ag1(t, u)

        @pl.when(jnp.logical_not(gather))
        def _():
            finish(t, u, post, False)

    def events(t, post, reduce, early, gather):
        def onward():
            rs3(t, 0)
            pl.when(jnp.logical_not(early))(lambda: rs2(t, 1))

        def if_reduce(what):
            return lambda: pl.when(reduce)(what)

        def if_gather(f, u):
            return lambda: pl.when(gather)(lambda: f(t, u))

        return (if_reduce(onward), if_reduce(lambda: settle(t, 0, post, gather)), if_reduce(lambda: rs3(t, 1)),
                if_reduce(lambda: settle(t, 1, post, gather)),
                if_gather(ag2, 0), if_gather(ag3, 0), if_gather(ag2, 1), if_gather(ag3, 1), if_gather(ag4, 0))

    def at(step, low, high, early, plan, todo):
        if DO_COMM:
            for (soon, late), what in sorted(zip(plan, todo), key=lambda e: e[0][1]):
                if low <= soon < high or low <= late < high:
                    pl.when(step == jnp.where(early, soon, late))(what)

    def rest(early, plan, todo, last):
        for (soon, late), what in zip(plan, todo):
            if max(soon, late) >= last:
                pl.when(jnp.where(early, soon, late) >= last)(what)

    def att_phase(l, s):
        t = 1 - s
        reduce = (l > 0) | (s > 0)
        early = l == 0
        todo = events(t, 4 * l - 1 + 2 * s, reduce, early, l >= 0)
        n_proj = n_q + 1
        n_out = dim // out_step
        first_block = 2 * n_proj
        per_half = 2 * heads + n_out
        last = first_block + 2 * per_half
        if DO_COMPUTE:
            for c in att_weight_copies(l)[:-1]:
                pl.when(s == 0)(c.wait)
        if DO_COMM:
            ag5(s, 0)

        def proj(i, carry):
            if DO_COMPUTE:
                pl.when(i % n_proj < n_q)(lambda: project_q(i % n_proj, i // n_proj, s))
                pl.when(i % n_proj == n_q)(lambda: project_kv(i // n_proj, s))
            if DO_COMM:
                pl.when(i == 0)(lambda: ag4(s, 1))

                @pl.when(i == n_proj - 1)
                def _():
                    ag5(s, 1)
                    ag_drain(s, (l == 0) & (s == 0))
            at(i, 0, first_block, early, ATT_PLAN, todo)
            return carry

        repeat(first_block, proj)
        if DO_COMPUTE:
            for c in fresh_out(s, l):
                c.start()
            for c in cache_copies(kl_hbm, vl_hbm, s):
                c.wait()
        for u in PAIR:
            low = first_block + u * per_half

            def blk(i, carry):
                if DO_COMPUTE:
                    pl.when(i % 2 == 0)(lambda: scores(i // 2, u, s, l))
                    pl.when(i % 2 == 1)(lambda: weigh(i // 2, u))
                at(low + i, low, low + 2 * heads, early, ATT_PLAN, todo)
                if DO_COMM and u == 1:
                    @pl.when(early & (i == 1))
                    def _():
                        ag_own(t)
                        swap_columns(s, 0, 0, dim)

                    @pl.when(early & (i == LEAVE))
                    def _():
                        rs1(s, 0)
                        rs2(s, 0)
                return carry

            repeat(2 * heads, blk)
            if DO_COMPUTE and u == 0:
                pl.when(s == 0)(att_weight_copies(l)[-1].wait)
            if DO_COMPUTE and u == 1:
                for c in fresh_out(s, l):
                    c.wait()

                @pl.when((l == 0) & (s == 0))
                def _():
                    for c in cache_copies(kl_hbm, vl_hbm, 1):
                        c.start()

                @pl.when(l + s == 1)
                def _():
                    for c in cache_copies(kg_hbm, vg_hbm, l):
                        c.start()
            if DO_COMM:
                if u == 1:
                    pl.when(jnp.logical_not(early))(lambda: ag_own(t))

            def out_body(i, carry):
                if DO_COMPUTE:
                    out_tile(i, u, s)
                for j in range(out_step // swap_step):
                    first = i * out_step + j * swap_step
                    if u == 1:
                        pl.when(jnp.logical_not(early))(lambda: swap_columns(s, 0, first, swap_step))
                        swap_columns(s, 1, first, swap_step)
                at(low + 2 * heads + i, low + 2 * heads, low + per_half, early, ATT_PLAN, todo)
                return carry

            repeat(n_out, out_body)
        if DO_COMPUTE:
            @pl.when((s == 1) & (l == 0))
            def _():
                for c in att_weight_copies(1):
                    c.start()
        if DO_COMM:
            @pl.when(early)
            def _():
                rs1(s, 1)
                rs2(s, 1)

            @pl.when(jnp.logical_not(early))
            def _():
                rs1(s, 0)
                rs2(s, 0)
                rs1(s, 1)
            rest(early, ATT_PLAN, todo, last)
            pl.when(reduce)(lambda: rs_drain(t))

    def mlp_phase(l, s):
        t = 1 - s
        m0 = (2 * l + s) * per_phase
        gather = (l == 0) | (s == 0)
        early = l + s == 0
        todo = events(t, 4 * l + 1 + 2 * s, l >= 0, early, gather)
        first_down = n_up + 2
        last = first_down + n_pairs
        if DO_COMM:
            ag5(s, 0)

        def halves(i, carry):
            if DO_COMPUTE:
                m = m0 + 2 * i

                @pl.when(i < 2)
                def _():
                    wait_up_tile(m % SLOTS)
                    wait_up_tile((m + 1) % SLOTS)
                up_half(i % 2, i // 2, s, m0)

                @pl.when(i >= 2)
                def _():
                    next_tile(m - 4)
                    next_tile(m - 3)
            if DO_COMM:
                pl.when(i == 0)(lambda: ag4(s, 1))

                @pl.when(i == 1)
                def _():
                    ag5(s, 1)
                    ag_drain(s, l < 0)
            at(i, 0, 4, early, MLP_PLAN, todo)
            return carry

        repeat(4, halves)

        def ups(jj, carry):
            if DO_COMPUTE:
                up_tile(jj, s, m0)
            at(2 + jj, 4, first_down, early, MLP_PLAN, todo)
            return carry

        repeat(n_up, ups, 2)

        every = swap_step // (DOWN * TILE)

        @pl.when(gather)
        def _():
            def downs(n, carry):
                if DO_COMPUTE:
                    down_pairs(n, 1, s, m0)
                if DO_COMM:
                    pl.when(n == every - 1)(lambda: ag_own(t))

                @pl.when(n % every == every - 1)
                def _():
                    for u in PAIR:
                        swap_columns(s, u, n // every * swap_step, swap_step)
                at(first_down + n, first_down, last, early, MLP_PLAN, todo)
                return carry

            repeat(n_pairs, downs)
            if DO_COMM:
                rs1(s, 0)
                rs2(s, 0)
                rs1(s, 1)
                rest(early, MLP_PLAN, todo, last)

        @pl.when(jnp.logical_not(gather))
        def _():
            if DO_COMM:
                rest(early, MLP_PLAN[:4], todo, first_down)
                for dev in partners:
                    pl.semaphore_signal(credit, inc=1, device_id=dev, device_id_type=MESH_ID)
            n_steps = n_pairs // GROUP
            rare = 1
            width = rare * GROUP * DOWN * TILE
            for u in PAIR:
                def downs(n, carry):
                    if DO_COMPUTE:
                        down_pairs(u * n_pairs + n * GROUP, GROUP, s, m0, u)
                    if DO_COMM:
                        if u == 0:
                            pl.when(n == rare - 1)(lambda: pl.semaphore_wait(credit, len(partners)))
                        pl.when(n % rare == rare - 1)(lambda: swap_columns(s, u, n // rare * width, width))
                        if u == 1:
                            @pl.when(n == 0)
                            def _():
                                rs1(s, 0)
                                rs2(s, 0)
                    return carry

                repeat(n_steps, downs)
            if DO_COMM:
                rs1(s, 1)
                rs3(s, 0)
                fold(s, 1, 1)
                fold(s, 1, 3)
                pl.delay(HOLD_NS)
                rs_right(s, 1, 1).start()
                rs_left(s, 1, 1).start()
        if DO_COMM:
            rs_drain(t)

    first = [pltpu.make_async_copy(src, dst, s_x.at[i]) for i, (src, dst) in enumerate(((x_hbm, xs), (norms_hbm, norms_ref), (freq_hbm, freq_ref)))]
    for copy in first:
        copy.start()
    barrier = pltpu.get_barrier_semaphore()
    for dev in partners:
        pl.semaphore_signal(barrier, inc=1, device_id=dev, device_id_type=MESH_ID)

    def first_norm(s, u):
        def body(hh, carry):
            v = xs[s, u, rows(hh)].astype(F32)
            g[s, me, u, rows(hh)] = (v * inv_rms(v) * (1.0 + norm_row(0))).astype(BF16)
            return carry

        repeat(2, body)

    for copy in first:
        copy.wait()
    first_norm(0, 0)
    pl.semaphore_wait(barrier, len(partners))
    for u in PAIR:
        if u == 1:
            first_norm(0, 1)
        if DO_COMM:
            ag_out(0, u, 0)
            ag_d2d(0, u, 0, core).start()
    if DO_COMPUTE:
        for c in att_weight_copies(0) + cache_copies(kl_hbm, vl_hbm, 0):
            c.start()
        for m in range(SLOTS):
            start_tile(jnp.int32(m))
    for u in PAIR:
        first_norm(1, u)
    for s in PAIR:
        shape = cos_ref.shape[1:]
        pos = start_ref[s] + sum(n * lax.broadcasted_iota(jnp.int32, shape, i) for i, n in enumerate((2 * half, half, 1)))
        angle = pos.astype(F32) * freq_ref[...]
        cos_ref[s] = jnp.cos(angle)
        sin = jnp.sin(angle)
        sin_ref[s] = jnp.where(lax.broadcasted_iota(jnp.int32, shape, 3) < hd // 2, -sin, sin)
        bias[s] = jnp.where(lax.broadcasted_iota(jnp.int32, (1, past), 1) < start_ref[s], 0.0, MASKED)
    if DO_COMM:
        for u in PAIR:
            ag_gone(0, u, 0)
            ag_out(0, u, 1)
        for u in PAIR:
            ag2(0, u)
        for u in PAIR:
            ag3(0, u)
        ag4(0, 0)
        ag_own(0)
        for u in PAIR:
            ag1(1, u)

    def layer(l, carry):
        def att(s, carry):
            att_phase(l, s)
            return carry

        def mlp(s, carry):
            mlp_phase(l, s)
            return carry

        repeat(2, att)
        repeat(2, mlp)
        return carry

    repeat(2, layer)

    out = [pltpu.make_async_copy(xs.at[s, u], xo_hbm.at[s, u], s_xo.at[s, u]) for s in PAIR for u in PAIR]
    out[0].start()
    out[1].start()
    for u in PAIR:
        if DO_COMM:
            if u == 1:
                rs3(1, 1)
            rs4_wait(1, u)
            finish(1, u, 7, False)
        out[2 + u].start()
    if DO_COMM:
        rs_drain(1)
    for copy in out:
        copy.wait()


def run_layers(x, start, freq, norms, kl, vl, kg, vg, wq, wk, wv, wo, wg, wu, wd):
    seqs, _, half, dim = x.shape
    _, past, hd = kl.shape
    chunk = kg.shape[1] - past
    n_q = wq.shape[2] // TILE
    devices = chunk // (2 * half)
    ring = pltpu.VMEM((2, 3, half // 2, dim), BF16)
    keys = pltpu.VMEM((past + chunk, hd), BF16)
    whole = pltpu.VMEM((2, devices, 2, half, dim), BF16)
    table = pltpu.VMEM((2, devices, 2, half, hd), F32)

    def dmas(*shape):
        return pltpu.SemaphoreType.DMA(shape)

    scratch = [
        whole, whole,
        pltpu.VMEM((4, 2, half, dim), BF16),
        ring, ring,
        pltpu.VMEM(x.shape, BF16),
        pltpu.VMEM(norms.shape, F32), pltpu.VMEM(freq.shape, F32),
        table, table,
        pltpu.VMEM((2, 1, past), F32),
        pltpu.VMEM((n_q + 1, dim, TILE), BF16),
        pltpu.VMEM(wo.shape[1:], BF16),
        pltpu.VMEM((SLOTS, max(dim, DOWN * wd.shape[1]), TILE), BF16),
        pltpu.VMEM((devices, 2, half, wg.shape[2]), BF16),
        pltpu.VMEM((wq.shape[2] // hd, devices, 2, half, hd), BF16),
        pltpu.VMEM((devices, 2, half, wq.shape[2]), BF16),
        keys, keys,
        pltpu.VMEM((chunk // 2, past + chunk), F32),
        pltpu.VMEM((chunk // 2, hd), F32),
        dmas(3), dmas(n_q + 3), dmas(SLOTS, DOWN), dmas(2), dmas(2), dmas(2, 2), pltpu.SemaphoreType.REGULAR,
    ]
    chips = [dmas(2, 2, 3)] * 2
    cores = [dmas(2, 2, 4)] * 2
    sends = [dmas(2, 2, 2, 3)]
    scratch += cores + chips + sends + sends + chips + cores
    return pl.pallas_call(
        layers_kernel,
        out_shape=(jax.ShapeDtypeStruct(x.shape, BF16),) + (jax.ShapeDtypeStruct((2, seqs, chunk, hd), BF16),) * 2,
        in_specs=[ANY, SMEM] + [ANY] * 13,
        out_specs=(ANY,) * 3,
        scratch_shapes=scratch,
        compiler_params=pltpu.CompilerParams(collective_id=0, has_side_effects=True, vmem_limit_bytes=LAYERS_LIMIT),
        name='layers',
    )(x, start, freq, norms, kl, vl, kg, vg, wq, wk, wv, wo, wg, wu, wd)


def cache_kernel(start_ref, x, k_new, v_new, kl, vl, kg, vg, x_o, kl_o, vl_o, kg_o, vg_o, xbuf, buf, fresh, turned, s_x, s_in, s_fr, s_out):
    _, _, chunk, _ = k_new.shape
    _, window, _ = kl.shape
    _, size, hd = fresh.shape
    lead = size - chunk
    jobs = []
    for b in PAIR:
        for l, group in enumerate((((kl, k_new, kl_o), (vl, v_new, vl_o)), ((kg, k_new, kg_o), (vg, v_new, vg_o)))):
            jobs += [(c, new, out, l, b) for c, new, out in group]
    rows_in = [pltpu.make_async_copy(new.at[l, b], fresh.at[i, pl.ds(0, chunk)], s_fr.at[i]) for i, (_, new, _, l, b) in enumerate(jobs)]
    loads = [pltpu.make_async_copy(c.at[b], buf.at[i, pl.ds(0, c.shape[1])], s_in.at[i]) for i, (c, _, _, _, b) in enumerate(jobs)]
    stores = [pltpu.make_async_copy(buf.at[i, pl.ds(0, c.shape[1])], out.at[b], s_out.at[i]) for i, (c, _, out, _, b) in enumerate(jobs)]
    x_in = pltpu.make_async_copy(x, xbuf, s_x)
    x_out = pltpu.make_async_copy(xbuf, x_o, s_x)
    for copy in rows_in + loads + [x_in]:
        copy.start()
    for i, (_, _, _, l, b) in enumerate(jobs):
        rows_in[i].wait()
        turned[i] = pltpu.roll(fresh[i].astype(F32), start_ref[b] % lead, 0).astype(BF16)
    row = lax.broadcasted_iota(jnp.int32, (lead, hd), 0)
    for i, (_, _, _, l, b) in enumerate(jobs):
        loads[i].wait()
        start = start_ref[b]
        r = start % lead
        at = pl.multiple_of(start - r, lead)
        end = pl.ds(pl.multiple_of(at + chunk, lead), lead)
        first = buf[i, pl.ds(at, lead)].astype(F32)
        after = buf[i, end].astype(F32)
        buf[i, pl.ds(at, lead)] = jnp.where(row >= r, turned[i, pl.ds(0, lead)].astype(F32), first).astype(BF16)
        buf[i, pl.ds(pl.multiple_of(at + lead, lead), chunk - lead)] = turned[i, pl.ds(lead, chunk - lead)]
        buf[i, end] = jnp.where(row < r, turned[i, pl.ds(chunk, lead)].astype(F32), after).astype(BF16)
        if l == 0:
            over = buf[i, pl.ds(window, chunk)].astype(F32)
            head = buf[i, pl.ds(0, chunk)].astype(F32)
            landed = lax.broadcasted_iota(jnp.int32, over.shape, 0) < start + chunk - window
            buf[i, pl.ds(0, chunk)] = jnp.where(landed, over, head).astype(BF16)
        stores[i].start()
    x_in.wait()
    x_out.start()
    for copy in stores + [x_out]:
        copy.wait()


def write_caches(start, x, k_new, v_new, kl, vl, kg, vg):
    _, _, hd = kl.shape
    _, _, chunk, _ = k_new.shape
    lead = 16
    depth = max(kl.shape[1] + chunk, kg.shape[1]) + lead
    jobs = 4 * len(PAIR)
    dmas = pltpu.SemaphoreType.DMA((jobs,))
    chunks = pltpu.VMEM((jobs, chunk + lead, hd), BF16)
    return pl.pallas_call(
        cache_kernel,
        out_shape=tuple(jax.ShapeDtypeStruct(c.shape, BF16) for c in (x, kl, vl, kg, vg)),
        in_specs=[SMEM] + [ANY] * 7,
        out_specs=(ANY,) * 5,
        scratch_shapes=[pltpu.VMEM(x.shape, BF16), pltpu.VMEM((jobs, depth, hd), BF16), chunks, chunks,
                        pltpu.SemaphoreType.DMA, dmas, dmas, dmas],
        compiler_params=pltpu.CompilerParams(vmem_limit_bytes=VMEM_LIMIT),
        name='write_caches',
    )(start, x, k_new, v_new, kl, vl, kg, vg)


def solution(mesh):
    act_spec = P('dp', 'tp', None)
    cache_spec = P('dp', None, 'tp', None)
    col_spec = P(None, None, 'tp')
    row_spec = P(None, 'tp', None)
    arg_specs = (act_spec, P('dp'), cache_spec, cache_spec, cache_spec, cache_spec, P(), col_spec, col_spec, col_spec, row_spec, col_spec, col_spec, row_spec)
    result_specs = (act_spec, cache_spec, cache_spec, cache_spec, cache_spec)

    def device_step(x, start, k_local, v_local, k_global, v_global, norms, w_q, w_k, w_v, w_o, w_gate, w_up, w_down):
        hd = k_local.shape[3]
        freq = ROPE_BASE ** (np.arange(hd // 2) * (-2.0 / hd))
        freq = jnp.asarray(np.concatenate([freq, freq])[None], F32)
        flat = [c.reshape(c.shape[0], c.shape[1], hd) for c in (k_local, v_local, k_global, v_global)]
        x4 = x.reshape(x.shape[0], 2, x.shape[1] // 2, x.shape[2])
        x_out, k_new, v_new = run_layers(x4, start, freq, norms, *flat, w_q, w_k, w_v, w_o, w_gate, w_up, w_down)
        x_out = x_out.reshape(x.shape)
        x_out, *caches = write_caches(start, x_out, k_new, v_new, *flat)
        return (x_out,) + tuple(c.reshape(c.shape[0], c.shape[1], 1, hd) for c in caches)

    return jax.shard_map(device_step, mesh=mesh, in_specs=arg_specs, out_specs=result_specs, check_vma=False)
```
